512 devices in a mesh: exp: 64 (over y, z), ctx: 8 (over x, core).
Axes of the slice: x: 4, y: 4, z: 16, core: 2. Of those that a mesh axis runs over, the one named last changes fastest.
Arguments:
- inputs: bfloat16 [65536, 1024], P(('exp', 'ctx')), may hold values from -30 to 30
- selected: int32 [128, 128], P(None, 'ctx'), may hold values from 0 to 65535, as said below
- selection_gate: float32 [128, 128], P('exp', 'ctx'), may hold values from 0.1 to 1
- gate_weight: bfloat16 [128, 1024, 2048], P('exp', None, 'ctx'), may hold values from -0.1875 to 0.1875
- up_weight: bfloat16 [128, 1024, 2048], P('exp', None, 'ctx'), may hold values from -0.1875 to 0.1875
- down_weight: bfloat16 [128, 2048, 1024], P('exp', 'ctx'), may hold values from -0.125 to 0.125
- norm_gain: float32 [1024], replicated, may hold values from 0.5 to 1.5
- query_weight: bfloat16 [1024, 1024], P('exp'), may hold values from -1 to 1
- key_weight: bfloat16 [1024, 1024], P('exp'), may hold values from -1 to 1
- value_weight: bfloat16 [1024, 1024], P('exp'), may hold values from -0.1875 to 0.1875
- train_count: int32 [64], P('exp'), may hold values from 256 to 1023
Outputs:
- layer_out: bfloat16 [65536, 1024], P(('exp', 'ctx'))
- context: bfloat16 [65536, 1024], P(('exp', 'ctx'))
The draws below stay inside these ranges and needn't reach their ends.
Inputs may be any that keep to these rules, and one draw needn't show every extreme that they name: `selected`: each expert's 128 entries are distinct rows. Entries c * 16 to (c + 1) * 16 - 1 of every expert name rows at positions c * 128 to (c + 1) * 128 - 1 of their tables. At most 2 entries of one expert name rows of one block of 128 rows, and in each group of 16 entries of each expert some block gives exactly 2.
All inputs are finite; a program needn't handle non-finite values.
Results may differ from the reference program's by a relative error of at most 0.017.
Values may be sent and summed in bfloat16 or wider, within the bound.
No kernel may reach another device: no remote copies, remote signals or barrier semaphores. Data moves between devices by JAX's collectives and lax.ppermute only.
A program may use at most 64 MiB of HBM per device.

```python
import jax
import jax.numpy as jnp
from jax import lax

D = 1024
FF = 2048
HEADS = 16
HEAD_DIM = 64
R_DEV = 128
GROUP_TAKE = 16
TABLES = 64
TABLE = 1024
ROWS = 65536
EXPERTS = 128
CAP = 128
MOST = 2
N_EXP = 64
N_CTX = 8


def log_even(key, grid_shape, low_end, high_end):
    return jnp.exp(jax.random.uniform(key, grid_shape, jnp.float32, jnp.log(low_end), jnp.log(high_end)))


def draw_inputs(key, part):
    key_list = jax.random.split(jax.random.fold_in(key, 21), 3)
    row_scale = log_even(key_list[0], (ROWS, 1), 0.3, 3.0)
    col_scale = log_even(key_list[1], (1, D), 0.3, 3.0)
    noise_part = jax.random.normal(key_list[2], (ROWS, D), jnp.float32)
    values = row_scale * col_scale * noise_part
    return jnp.clip(values, -30.0, 30.0).astype(jnp.bfloat16)


def drawn_weight(key, salt):
    base_matrix = jax.random.normal(jax.random.fold_in(key, salt), (D, D), jnp.float32) * D ** (-0.5)
    return jnp.clip(base_matrix, -1.0, 1.0).astype(jnp.bfloat16)


def draw_query_weight(key, part):
    return drawn_weight(key, 51)


def draw_key_weight(key, part):
    return drawn_weight(key, 52)


def draw_selected(key, part):
    key_list = jax.random.split(jax.random.fold_in(key, 41), 7)
    token_total = N_EXP * MOST
    grid_shape = (EXPERTS, N_CTX)
    hot_table = jnp.minimum(jax.random.randint(key_list[0], grid_shape, 0, N_EXP), jax.random.randint(key_list[1], grid_shape, 0, N_EXP))
    busy_level = jax.random.randint(key_list[2], (N_EXP,), 0, 4)
    token_index = jnp.arange(token_total, dtype=jnp.int32)
    token_table = token_index // MOST
    token_copy = token_index % MOST
    noise_part = jax.random.randint(key_list[3], grid_shape + (token_total,), 0, 65536)
    score_int = jnp.where(token_table[None, None, :] == hot_table[:, :, None], 1 << 30, 0) + jnp.take(busy_level, token_table)[None, None, :] * (1 << 28) + noise_part * 4096 + token_index[None, None, :]
    chosen = lax.top_k(score_int, GROUP_TAKE)[1].astype(jnp.int32)
    table_id = chosen // MOST
    copy_id = jnp.take(token_copy, chosen)
    offset_all = jax.random.randint(key_list[4], grid_shape + (N_EXP,), 0, R_DEV)
    stride_all = jax.random.randint(key_list[5], grid_shape + (N_EXP,), 1, R_DEV // MOST + 1)
    offset_pick = jnp.take_along_axis(offset_all, table_id, axis=2)
    stride_pick = jnp.take_along_axis(stride_all, table_id, axis=2)
    local_row = (offset_pick + copy_id * stride_pick) % R_DEV
    group_id = jnp.arange(N_CTX, dtype=jnp.int32)[None, :, None]
    row_ids = (table_id * N_CTX + group_id) * R_DEV + local_row
    shuffle_key = jax.random.randint(key_list[6], grid_shape + (GROUP_TAKE,), 0, 65536) * 1024 + jnp.arange(GROUP_TAKE, dtype=jnp.int32)
    shuffle_order = lax.top_k(shuffle_key, GROUP_TAKE)[1]
    row_ids = jnp.take_along_axis(row_ids, shuffle_order, axis=2)
    return row_ids.reshape(EXPERTS, CAP).astype(jnp.int32)


def set_ends(drawn, own_key, smallest, high):
    spot = [jax.random.randint(jax.random.fold_in(own_key, axis), (), 0, length) for axis, length in enumerate(drawn.shape)]
    longest = drawn.shape.index(max(drawn.shape))
    neighbour = spot[:longest] + [(spot[longest] + 1) % drawn.shape[longest]] + spot[longest + 1:]
    return drawn.at[tuple(spot)].set(smallest).at[tuple(neighbour)].set(high)


def block_scale(key, dims, shards, smallest, top_value):
    level, own = 1.0, jax.random.fold_in(key, 6)
    for dim, parts in shards:
        steps = jnp.exp(jax.random.uniform(jax.random.fold_in(own, dim), (parts,), jnp.float32, smallest / len(shards), top_value / len(shards)))
        level = level * jnp.repeat(steps, dims[dim] // parts).reshape([-1 if axis == dim else 1 for axis in range(len(dims))])
    return level


def scatter_about(key, extent, scale, limit, pieces=(), kind=jnp.bfloat16):
    values = scale * jax.random.normal(key, extent, jnp.float32)
    if pieces:
        values = values * block_scale(key, extent, pieces, -0.22, 0.18)
    return jnp.clip(values, -limit, limit).astype(kind)


def setup_inputs(seed: int = 0) -> dict:
    key_of = jax.random.split(jax.random.key(seed), 12)
    return {
        "inputs": draw_inputs(jax.random.fold_in(key_of[11], 71), 0),
        "selected": draw_selected(jax.random.fold_in(key_of[11], 71), 0),
        "selection_gate": jnp.clip(0.1 + 0.9 * jax.random.uniform(key_of[2], (EXPERTS, CAP), jnp.float32) ** block_scale(key_of[2], (EXPERTS, CAP), ((0, 64), (1, 8)), -0.2, 0.2), 0.1, 1.0),
        "gate_weight": scatter_about(key_of[3], (EXPERTS, D, FF), D ** -0.5, 0.1875, ((0, 64), (2, 8))),
        "up_weight": scatter_about(key_of[4], (EXPERTS, D, FF), D ** -0.5, 0.1875, ((0, 64), (2, 8))),
        "down_weight": scatter_about(key_of[5], (EXPERTS, FF, D), FF ** -0.5, 0.125, ((0, 64), (1, 8))),
        "norm_gain": jnp.clip(1.0 + 0.1 * jax.random.normal(key_of[6], (D,), jnp.float32), 0.5, 1.5),
        "query_weight": draw_query_weight(jax.random.fold_in(key_of[11], 71), 0),
        "key_weight": draw_key_weight(jax.random.fold_in(key_of[11], 71), 0),
        "value_weight": scatter_about(key_of[9], (D, D), D ** -0.5, 0.1875, ((0, 64),)),
        "train_count": set_ends(jax.random.randint(key_of[10], (TABLES,), TABLE // 4, TABLE), jax.random.fold_in(key_of[10], 1), TABLE // 4, TABLE - 1).astype(jnp.int32),
    }


EPSILON = 1e-06
MASKED = -1e+30

def expert_terms(inputs, selected, selection_gate, gate_weight, up_weight, down_weight):

    def one_expert(operands):
        chosen_rows, gate_row, gate_matrix, up_matrix, down_matrix = operands
        chosen = jnp.take(inputs, chosen_rows, axis=0)
        gate_part = jnp.dot(chosen, gate_matrix, preferred_element_type=jnp.float32)
        up_part = jnp.dot(chosen, up_matrix, preferred_element_type=jnp.float32)
        hidden = (jax.nn.silu(gate_part) * up_part).astype(jnp.bfloat16)
        expert_out = jnp.dot(hidden, down_matrix, preferred_element_type=jnp.float32)
        return (gate_row[:, None] * expert_out).astype(jnp.bfloat16)
    return lax.map(one_expert, (selected, selection_gate, gate_weight, up_weight, down_weight))

def table_attention(operands, norm_gain, query_weight, key_weight, value_weight):
    table_rows, train_rows = operands
    widened = table_rows.astype(jnp.float32)
    scale_row = lax.rsqrt(lax.optimization_barrier(jnp.mean(widened * widened, axis=1, keepdims=True)) + EPSILON)
    normed = (widened * scale_row * norm_gain).astype(jnp.bfloat16)
    query_rows = jnp.dot(normed, query_weight, preferred_element_type=jnp.float32).astype(jnp.bfloat16)
    key_rows = jnp.dot(normed, key_weight, preferred_element_type=jnp.float32).astype(jnp.bfloat16)
    value_rows = jnp.dot(normed, value_weight, preferred_element_type=jnp.float32).astype(jnp.bfloat16)
    query_heads = query_rows.astype(jnp.float32).reshape(TABLE, HEADS, HEAD_DIM)
    key_heads = key_rows.astype(jnp.float32).reshape(TABLE, HEADS, HEAD_DIM)
    value_heads = value_rows.astype(jnp.float32).reshape(TABLE, HEADS, HEAD_DIM)
    scores = jnp.einsum('qhd,khd->hqk', query_heads, key_heads) * HEAD_DIM ** (-0.5)
    allowed = jnp.arange(TABLE, dtype=jnp.int32) < train_rows
    scores = jnp.where(allowed, scores, MASKED)
    top_score = lax.optimization_barrier(jnp.max(scores, axis=2, keepdims=True))
    raw_weights = jnp.where(allowed, jnp.exp(scores - top_score), 0.0)
    denominator = lax.optimization_barrier(jnp.sum(raw_weights, axis=2))
    rounded = lax.optimization_barrier(raw_weights.astype(jnp.bfloat16)).astype(jnp.float32)
    context = jnp.einsum('hqk,khd->hqd', rounded, value_heads) / denominator[:, :, None]
    return jnp.transpose(context, (1, 0, 2)).reshape(TABLE, D).astype(jnp.bfloat16)

def reference(inputs, selected, selection_gate, gate_weight, up_weight, down_weight, norm_gain, query_weight, key_weight, value_weight, train_count):
    weighted = expert_terms(inputs, selected, selection_gate, gate_weight, up_weight, down_weight)
    moe_sum = jax.ops.segment_sum(weighted.reshape(-1, D).astype(jnp.float32), selected.reshape(-1), num_segments=ROWS)
    layer_out = (inputs.astype(jnp.float32) + moe_sum).astype(jnp.bfloat16)

    def per_table(operands):
        return table_attention(operands, norm_gain, query_weight, key_weight, value_weight)
    context = lax.map(per_table, (layer_out.reshape(TABLES, TABLE, D), train_count))
    return (layer_out, context.reshape(ROWS, D))
```

```python
import jax
import jax.numpy as jnp
from jax import lax
from jax.experimental import pallas as pl
from jax.experimental.pallas import tpu as pltpu
from jax.sharding import PartitionSpec as P

HEADS = 16
HEAD_DIM = 64
EPSILON = 1e-06
MASKED = -1e30
LOG2_E = 1.4426950408889634
MOST = 2

N_Z = 16
N_X, N_CORE = 4, 2

def exchange(blocks, axis):
    return lax.all_to_all(blocks, axis, split_axis=0, concat_axis=0, tiled=True)


def copies(shard, count):
    return jnp.broadcast_to(shard, (count, *shard.shape))


def shift(v, axis, move):
    count = lax.axis_size(axis)
    return lax.ppermute(v, axis, [(i, move(i)) for i in range(count)])


def shift_chip(v, step):
    return shift(v, "ctx", lambda i: (i // N_CORE + step) % N_X * N_CORE + i % N_CORE)


def swap_core(v):
    return shift(v, "ctx", lambda i: i ^ 1)


def gather_four(v, digit, stride):
    def move(step):
        return lambda i: i + ((i // stride + step) % 4 - i // stride % 4) * stride

    one, two, three = (shift(v, "exp", move(step)) for step in (1, 2, 3))
    turned = jnp.stack([three, two, one, v, three, two, one])
    return lax.dynamic_slice_in_dim(turned, 3 - digit, 4, 0)


def attention_kernel(ids, train, near, far, out, queries, keys, values, bias):
    chunks, rows = near.shape[0] // 128 * 2, 128
    half = chunks // 2
    width = 2 * HEAD_DIM
    lane = lax.broadcasted_iota(jnp.int32, (rows, width), 1)
    first = lane < HEAD_DIM
    for j in range(chunks):
        source = near if j < half else far
        at = (j % half) * rows
        queries[j] = source[pl.ds(at, rows), 0:width]
        keys[pl.ds(j * rows, rows), :] = source[pl.ds(at, rows), width : 2 * width]
        values[pl.ds(j * rows, rows), :] = source[pl.ds(at, rows), 2 * width : 3 * width]
        position = ids[j] * rows + lax.broadcasted_iota(jnp.int32, (1, rows), 1)
        bias[:, j * rows : (j + 1) * rows] = jnp.where(position < train[0], 0.0, MASKED)

    def one_chunk(j, carry):
        q = queries[j]
        zero = jnp.zeros_like(q)
        parts = []
        for h in range(2):
            q_h = jnp.where(first, q, zero) if h == 0 else jnp.where(first, zero, q)
            scores = lax.dot_general(
                q_h, keys[...], (((1,), (1,)), ((), ())), preferred_element_type=jnp.float32
            )
            scores = scores * (LOG2_E * HEAD_DIM**-0.5) + bias[...]
            top = jnp.max(scores, axis=1, keepdims=True)
            weights = jnp.exp2(scores - top)
            total = jnp.sum(weights, axis=1, keepdims=True)
            mixed = jnp.dot(
                weights.astype(jnp.bfloat16), values[...], preferred_element_type=jnp.float32
            )
            parts.append(mixed / total)
        out[ids[j]] = jnp.where(first, parts[0], parts[1]).astype(jnp.bfloat16)
        return carry

    lax.fori_loop(0, chunks, one_chunk, 0)


def attention(ids, train, near, far):
    chunks = ids.shape[0]
    rows, width = 128, 2 * HEAD_DIM
    vmem = pl.BlockSpec(memory_space=pltpu.VMEM)
    smem = pl.BlockSpec(memory_space=pltpu.SMEM)
    return pl.pallas_call(
        attention_kernel,
        out_shape=jax.ShapeDtypeStruct((chunks, rows, width), jnp.bfloat16),
        in_specs=[smem, smem, vmem, vmem],
        out_specs=vmem,
        scratch_shapes=[
            pltpu.VMEM((chunks, rows, width), jnp.bfloat16),
            pltpu.VMEM((chunks * rows, width), jnp.bfloat16),
            pltpu.VMEM((chunks * rows, width), jnp.bfloat16),
            pltpu.VMEM((1, chunks * rows), jnp.float32),
        ],
        name="attention",
    )(ids, train, near, far)


def local(
    inputs,
    selected,
    selection_gate,
    gate_weight,
    up_weight,
    down_weight,
    norm_gain,
    query_weight,
    key_weight,
    value_weight,
    train_count,
):
    exp_count = lax.axis_size("exp")
    ctx_count = lax.axis_size("ctx")
    exp_index = lax.axis_index("exp")
    ctx_index = lax.axis_index("ctx")
    row_count, model_width = inputs.shape
    experts = gate_weight.shape[0]
    group_take = selected.shape[1]
    table_rows = row_count * ctx_count
    head_width = model_width // ctx_count

    piece = jnp.concatenate(
        [
            lax.dynamic_slice_in_dim(w, ctx_index * head_width, head_width, 1)
            for w in (query_weight, key_weight, value_weight)
        ],
        axis=1,
    )
    own_block = exp_index * ctx_count + ctx_index
    taken = selected.reshape(exp_count, experts, group_take) - own_block * row_count
    mine = (taken >= 0) & (taken < row_count)
    lower = jnp.min(jnp.where(mine, taken, row_count), axis=2)
    upper = jnp.max(jnp.where(mine, taken, -1), axis=2)
    upper = jnp.where(upper > lower, upper, -1)
    picks = jnp.stack([lower, upper], axis=2)
    row_ids = jnp.arange(row_count, dtype=jnp.int32)
    owner_hit = (picks.reshape(-1, 1) == row_ids).astype(jnp.bfloat16)
    outgoing = jnp.dot(owner_hit, inputs, preferred_element_type=jnp.float32)
    outgoing = outgoing.astype(jnp.bfloat16).reshape(exp_count, -1, model_width)

    outgoing, piece = lax.optimization_barrier((outgoing, piece))
    quarter = gather_four(piece, exp_index // 4 % 4, 4)
    arrived = exchange(outgoing, "exp").reshape(-1, model_width)

    my_rows = lax.dynamic_slice_in_dim(selected, exp_index * experts, experts, 0)
    my_table = my_rows // table_rows
    lower_rows = (my_table[:, :, None] == my_table[:, None, :]) & (
        my_rows[:, None, :] < my_rows[:, :, None]
    )
    my_rank = jnp.sum(lower_rows.astype(jnp.int32), axis=2)
    expert_ids = jnp.arange(experts, dtype=jnp.int32)[:, None]
    my_place = ((my_table * experts + expert_ids) * MOST + my_rank).reshape(-1, 1)
    places = jnp.arange(exp_count * experts * MOST, dtype=jnp.int32)
    slot_hit = (my_place == places).astype(jnp.bfloat16)

    compact = jnp.dot(slot_hit, arrived, preferred_element_type=jnp.float32).astype(jnp.bfloat16)
    compact, quarter = lax.optimization_barrier((compact, quarter))
    layer = gather_four(quarter, exp_index % 4, 1)
    layer = jnp.moveaxis(layer, 0, 1)
    chosen = exchange(copies(compact, ctx_count), "ctx")
    chosen = chosen.reshape(ctx_count, experts, group_take, model_width)
    partials = []
    for x in range(experts):
        rows = chosen[:, x].reshape(-1, model_width)
        gate_part = jnp.dot(rows, gate_weight[x], preferred_element_type=jnp.float32)
        up_part = jnp.dot(rows, up_weight[x], preferred_element_type=jnp.float32)
        hidden = (jax.nn.silu(gate_part) * up_part).astype(jnp.bfloat16)
        partial = jnp.dot(hidden, down_weight[x], preferred_element_type=jnp.float32)
        partials.append(
            partial.astype(jnp.bfloat16).reshape(ctx_count, group_take, model_width)
        )
    parts = exchange(jnp.concatenate(partials, axis=1), "ctx")
    expert_out = jnp.sum(parts.astype(jnp.float32), axis=0)
    weighted = (expert_out * selection_gate.reshape(-1, 1)).astype(jnp.bfloat16)
    reply = lax.dot_general(
        slot_hit, weighted, (((0,), (0,)), ((), ())), preferred_element_type=jnp.float32
    )
    reply = reply.astype(jnp.bfloat16).reshape(exp_count, -1, model_width)
    reply, layer = lax.optimization_barrier((reply, layer))
    weight_rows = gather_four(layer, exp_index // N_Z, N_Z).reshape(model_width, -1)
    returned = exchange(reply, "exp").reshape(-1, model_width)
    moe_sum = lax.dot_general(
        owner_hit, returned, (((0,), (0,)), ((), ())), preferred_element_type=jnp.float32
    )

    layer_out = (inputs.astype(jnp.float32) + moe_sum).astype(jnp.bfloat16)
    widened = layer_out.astype(jnp.float32)
    scale_row = lax.rsqrt(jnp.mean(widened * widened, axis=1, keepdims=True) + EPSILON)
    normed = (widened * scale_row * norm_gain).astype(jnp.bfloat16)

    near = jnp.concatenate(
        [normed, shift_chip(normed, 1), shift_chip(normed, -1), shift_chip(normed, 2)], axis=0
    )
    far = swap_core(near)
    chip, core = ctx_index // N_CORE, ctx_index % N_CORE
    steps = jnp.array([0, N_X - 1, 1, 2], jnp.int32)
    chips = (chip + steps) % N_X
    ids = jnp.concatenate([chips * N_CORE + core, chips * N_CORE + 1 - core])
    near_rows = jnp.dot(near, weight_rows, preferred_element_type=jnp.float32)
    far_rows = jnp.dot(far, weight_rows, preferred_element_type=jnp.float32)
    mixed = attention(
        ids, train_count, near_rows.astype(jnp.bfloat16), far_rows.astype(jnp.bfloat16)
    )
    by_heads = exchange(mixed, "ctx")
    context = jnp.moveaxis(by_heads, 0, 1).reshape(row_count, model_width)
    return (layer_out, context)


def solution(mesh):
    placed = (
        P(("exp", "ctx"), None),
        P(None, "ctx"),
        P("exp", "ctx"),
        P("exp", None, "ctx"),
        P("exp", None, "ctx"),
        P("exp", "ctx", None),
        P(),
        P("exp", None),
        P("exp", None),
        P("exp", None),
        P("exp"),
    )
    return jax.shard_map(
        local,
        mesh=mesh,
        in_specs=placed,
        out_specs=(P(("exp", "ctx"), None), P(("exp", "ctx"), None)),
        check_vma=False,
    )
```

```python
import jax
import jax.numpy as jnp
from jax import lax
from jax.experimental import pallas as pl
from jax.experimental.pallas import tpu as pltpu
from jax.sharding import PartitionSpec as P


HEAD_DIM = 64
EPSILON = 1e-06
MASKED = -1e30
LOG2_E = 1.4426950408889634
MOST = 2

N_Z = 16
N_X, N_CORE = 4, 2


def exchange(blocks, axis):
    return lax.all_to_all(blocks, axis, split_axis=0, concat_axis=0, tiled=True)


def copies(shard, count):
    return jnp.broadcast_to(shard, (count, *shard.shape))


def shift(v, axis, move):
    count = lax.axis_size(axis)
    return lax.ppermute(v, axis, [(i, move(i)) for i in range(count)])


def shift_chip(v, step):
    return shift(v, "ctx", lambda i: (i // N_CORE + step) % N_X * N_CORE + i % N_CORE)


def swap_core(v):
    return shift(v, "ctx", lambda i: i ^ 1)


def gather_four(v, digit, stride):
    def move(step):
        return lambda i: i + ((i // stride + step) % 4 - i // stride % 4) * stride

    others = []
    for step in (1, 2, 3):
        others.append(shift(v, "exp", move(step)))
    one, two, three = others
    turned = jnp.stack([three, two, one, v, three, two, one])
    return lax.dynamic_slice_in_dim(turned, 3 - digit, 4, 0)


def expert_kernel(chosen, gate, up, down, out):
    senders, _, width = chosen.shape
    experts = gate.shape[0]
    take = chosen.shape[1] // experts
    for x in range(experts):
        slots = slice(x * take, (x + 1) * take)
        rows = chosen[:, slots, :].reshape(senders * take, width)
        gate_part = jnp.dot(rows, gate[x], preferred_element_type=jnp.float32)
        up_part = jnp.dot(rows, up[x], preferred_element_type=jnp.float32)
        hidden = (gate_part / (1.0 + jnp.exp(-gate_part)) * up_part).astype(jnp.bfloat16)
        partial = jnp.dot(hidden, down[x], preferred_element_type=jnp.float32)
        out[:, slots, :] = partial.astype(jnp.bfloat16).reshape(senders, take, width)


def expert_parts(chosen, gate, up, down):
    vmem = pl.BlockSpec(memory_space=pltpu.VMEM)
    return pl.pallas_call(
        expert_kernel,
        out_shape=jax.ShapeDtypeStruct(chosen.shape, chosen.dtype),
        in_specs=[vmem] * 4,
        out_specs=vmem,
        compiler_params=pltpu.CompilerParams(vmem_limit_bytes=12 * 2**20),
        name="experts",
    )(chosen, gate, up, down)


def attention_kernel(ids, train, near, far, out, queries, keys, values):
    rows, width = 128, 2 * HEAD_DIM
    half = near.shape[0] // rows
    chunks = 2 * half
    lane = lax.broadcasted_iota(jnp.int32, (rows, width), 1)
    first = lane < HEAD_DIM
    one_lane = jnp.where(lane == 0, 1.0, 0.0).astype(jnp.bfloat16)
    for j in range(chunks):
        source = near if j < half else far
        at = (j % half) * rows
        here = slice(j * rows, (j + 1) * rows)
        low, high = slice(2 * j * rows, (2 * j + 1) * rows), slice((2 * j + 1) * rows, (2 * j + 2) * rows)
        q = source[at : at + rows, 0:width]
        zero = jnp.zeros_like(q)
        queries[low, 0:width] = jnp.where(first, q, zero)
        queries[high, 0:width] = jnp.where(first, zero, q)
        queries[low, width:] = one_lane
        queries[high, width:] = one_lane
        position = ids[j] * rows + lax.broadcasted_iota(jnp.int32, (rows, width), 0)
        masked = (position >= train[0]) & (lane == 0)
        keys[here, 0:width] = source[at : at + rows, width : 2 * width]
        keys[here, width:] = jnp.where(masked, MASKED, 0.0).astype(jnp.bfloat16)
        values[here, 0:width] = source[at : at + rows, 2 * width : 3 * width]
        values[here, width:] = jnp.ones((rows, width), jnp.bfloat16)

    for j in range(chunks):
        q = queries[2 * j * rows : (2 * j + 2) * rows, :]
        scores = lax.dot_general(
            q, keys[...], (((1,), (1,)), ((), ())), preferred_element_type=jnp.float32
        )
        top = jnp.max(scores, axis=1, keepdims=True)
        weights = jnp.exp2((scores - top) * (LOG2_E * HEAD_DIM**-0.5)).astype(jnp.bfloat16)
        mixed = jnp.dot(weights, values[...], preferred_element_type=jnp.float32)
        blended = mixed[:, :width] / mixed[:, width:]
        out[ids[j]] = jnp.where(first, blended[:rows], blended[rows:]).astype(jnp.bfloat16)


def attention(ids, train, near, far):
    chunks = ids.shape[0]
    rows, width = 128, 2 * HEAD_DIM
    vmem = pl.BlockSpec(memory_space=pltpu.VMEM)
    smem = pl.BlockSpec(memory_space=pltpu.SMEM)
    return pl.pallas_call(
        attention_kernel,
        out_shape=jax.ShapeDtypeStruct((chunks, rows, width), jnp.bfloat16),
        in_specs=[smem, smem, vmem, vmem],
        out_specs=vmem,
        scratch_shapes=[
            pltpu.VMEM((2 * chunks * rows, 2 * width), jnp.bfloat16),
            pltpu.VMEM((chunks * rows, 2 * width), jnp.bfloat16),
            pltpu.VMEM((chunks * rows, 2 * width), jnp.bfloat16),
        ],
        compiler_params=pltpu.CompilerParams(vmem_limit_bytes=20 * 2**20),
        name="attention",
    )(ids, train, near, far)


def local(
    inputs,
    selected,
    selection_gate,
    gate_weight,
    up_weight,
    down_weight,
    norm_gain,
    query_weight,
    key_weight,
    value_weight,
    train_count,
):
    exp_count = lax.axis_size("exp")
    ctx_count = lax.axis_size("ctx")
    exp_index = lax.axis_index("exp")
    ctx_index = lax.axis_index("ctx")
    row_count, model_width = inputs.shape
    experts = gate_weight.shape[0]
    group_take = selected.shape[1]
    table_rows = row_count * ctx_count
    head_width = model_width // ctx_count

    piece = jnp.concatenate(
        [
            lax.dynamic_slice_in_dim(w, ctx_index * head_width, head_width, 1)
            for w in (query_weight, key_weight, value_weight)
        ],
        axis=1,
    )
    own_block = exp_index * ctx_count + ctx_index
    taken = selected.reshape(exp_count, experts, group_take) - own_block * row_count
    mine = (taken >= 0) & (taken < row_count)
    lower = jnp.min(jnp.where(mine, taken, row_count), axis=2)
    upper = jnp.max(jnp.where(mine, taken, -1), axis=2)
    upper = jnp.where(upper > lower, upper, -1)
    picks = jnp.stack([lower, upper], axis=2)
    row_ids = jnp.arange(row_count, dtype=jnp.int32)
    owner_hit = (picks.reshape(-1, 1) == row_ids).astype(jnp.bfloat16)
    outgoing = jnp.dot(owner_hit, inputs, preferred_element_type=jnp.float32)
    outgoing = outgoing.astype(jnp.bfloat16).reshape(exp_count, -1, model_width)

    arrived = exchange(outgoing, "exp").reshape(-1, model_width)

    my_rows = lax.dynamic_slice_in_dim(selected, exp_index * experts, experts, 0)
    my_table = my_rows // table_rows
    lower_rows = (my_table[:, :, None] == my_table[:, None, :]) & (
        my_rows[:, None, :] < my_rows[:, :, None]
    )
    my_rank = jnp.sum(lower_rows.astype(jnp.int32), axis=2)
    expert_ids = jnp.arange(experts, dtype=jnp.int32)[:, None]
    my_place = ((my_table * experts + expert_ids) * MOST + my_rank).reshape(-1, 1)
    places = jnp.arange(exp_count * experts * MOST, dtype=jnp.int32)
    slot_hit = (my_place == places).astype(jnp.bfloat16)

    compact = jnp.dot(slot_hit, arrived, preferred_element_type=jnp.float32).astype(jnp.bfloat16)
    compact, piece = lax.optimization_barrier((compact, piece))
    quarter = gather_four(piece, exp_index // 4 % 4, 4)
    chosen = exchange(copies(compact, ctx_count), "ctx")
    partials = expert_parts(chosen, gate_weight, up_weight, down_weight)
    partials, quarter = lax.optimization_barrier((partials, quarter))
    layer = jnp.moveaxis(gather_four(quarter, exp_index % 4, 1), 0, 1)
    parts = exchange(partials, "ctx")
    expert_out = jnp.sum(parts.astype(jnp.float32), axis=0)
    weighted = (expert_out * selection_gate.reshape(-1, 1)).astype(jnp.bfloat16)
    reply = lax.dot_general(
        slot_hit, weighted, (((0,), (0,)), ((), ())), preferred_element_type=jnp.float32
    )
    reply = reply.astype(jnp.bfloat16).reshape(exp_count, -1, model_width)
    reply, layer = lax.optimization_barrier((reply, layer))
    weight_rows = gather_four(layer, exp_index // N_Z, N_Z).reshape(model_width, -1)
    returned = exchange(reply, "exp")
    returned = returned.reshape(-1, model_width)
    moe_sum = lax.dot_general(
        owner_hit, returned, (((0,), (0,)), ((), ())), preferred_element_type=jnp.float32
    )

    layer_out = (inputs.astype(jnp.float32) + moe_sum).astype(jnp.bfloat16)
    widened = layer_out.astype(jnp.float32)
    scale_row = lax.rsqrt(jnp.mean(widened * widened, axis=1, keepdims=True) + EPSILON)
    normed = (widened * scale_row * norm_gain).astype(jnp.bfloat16)

    near = jnp.concatenate(
        [normed, shift_chip(normed, 1), shift_chip(normed, -1), shift_chip(normed, 2)], axis=0
    )
    far = swap_core(near)
    chip, core = ctx_index // N_CORE, ctx_index % N_CORE
    steps = jnp.array([0, N_X - 1, 1, 2], jnp.int32)
    chips = (chip + steps) % N_X
    ids = jnp.concatenate([chips * N_CORE + core, chips * N_CORE + 1 - core])
    near_rows = jnp.dot(near, weight_rows, preferred_element_type=jnp.float32)
    far_rows = jnp.dot(far, weight_rows, preferred_element_type=jnp.float32)
    mixed = attention(
        ids, train_count, near_rows.astype(jnp.bfloat16), far_rows.astype(jnp.bfloat16)
    )
    by_heads = exchange(mixed, "ctx")
    context = jnp.moveaxis(by_heads, 0, 1).reshape(row_count, model_width)
    return (layer_out, context)


def solution(mesh):
    placed = (
        P(("exp", "ctx"), None),
        P(None, "ctx"),
        P("exp", "ctx"),
        P("exp", None, "ctx"),
        P("exp", None, "ctx"),
        P("exp", "ctx", None),
        P(),
        P("exp", None),
        P("exp", None),
        P("exp", None),
        P("exp"),
    )
    return jax.shard_map(
        local,
        mesh=mesh,
        in_specs=placed,
        out_specs=(P(("exp", "ctx"), None), P(("exp", "ctx"), None)),
        check_vma=False,
    )
```

```python
import jax
import jax.numpy as jnp
from jax import lax
from jax.experimental import pallas as pl
from jax.experimental.pallas import tpu as pltpu
from jax.sharding import PartitionSpec as P


HEAD_DIM = 64
EPSILON = 1e-06
MASKED = -1e30
LOG2_E = 1.4426950408889634
MOST = 2

N_Z = 16
N_X, N_CORE = 4, 2


def exchange(blocks, axis):
    return lax.all_to_all(blocks, axis, split_axis=0, concat_axis=0, tiled=True)


def copies(shard, count):
    return jnp.broadcast_to(shard, (count, *shard.shape))


def shift(v, axis, move):
    count = lax.axis_size(axis)
    return lax.ppermute(v, axis, [(i, move(i)) for i in range(count)])


def shift_chip(v, step):
    return shift(v, "ctx", lambda i: (i // N_CORE + step) % N_X * N_CORE + i % N_CORE)


def swap_core(v):
    return shift(v, "ctx", lambda i: i ^ 1)


def gather_four(v, digit, stride):
    def move(step):
        return lambda i: i + ((i // stride + step) % 4 - i // stride % 4) * stride

    others = []
    for step in (1, 2, 3):
        others.append(shift(v, "exp", move(step)))
    one, two, three = others
    turned = jnp.stack([three, two, one, v, three, two, one])
    return lax.dynamic_slice_in_dim(turned, 3 - digit, 4, 0)


def expert_kernel(chosen, gate, up, down, out, down_here, sems):
    senders, _, width = chosen.shape
    experts = gate.shape[0]
    take = chosen.shape[1] // experts
    moves = [
        pltpu.make_async_copy(down.at[x], down_here.at[x], sems.at[x]) for x in range(experts)
    ]
    for move in moves:
        move.start()
    for x in range(experts):
        slots = slice(x * take, (x + 1) * take)
        rows = chosen[:, slots, :].reshape(senders * take, width)
        gate_part = jnp.dot(rows, gate[x], preferred_element_type=jnp.float32)
        up_part = jnp.dot(rows, up[x], preferred_element_type=jnp.float32)
        hidden = (gate_part / (1.0 + jnp.exp(-gate_part)) * up_part).astype(jnp.bfloat16)
        moves[x].wait()
        partial = jnp.dot(hidden, down_here[x], preferred_element_type=jnp.float32)
        out[:, slots, :] = partial.astype(jnp.bfloat16).reshape(senders, take, width)


def expert_parts(chosen, gate, up, down):
    vmem = pl.BlockSpec(memory_space=pltpu.VMEM)
    return pl.pallas_call(
        expert_kernel,
        out_shape=jax.ShapeDtypeStruct(chosen.shape, chosen.dtype),
        in_specs=[vmem, vmem, vmem, pl.BlockSpec(memory_space=pltpu.HBM)],
        out_specs=vmem,
        scratch_shapes=[
            pltpu.VMEM(down.shape, down.dtype),
            pltpu.SemaphoreType.DMA((down.shape[0],)),
        ],
        compiler_params=pltpu.CompilerParams(vmem_limit_bytes=12 * 2**20),
        name="experts",
    )(chosen, gate, up, pltpu.with_memory_space_constraint(down, pltpu.HBM))


def attention_kernel(ids, train, near, far, out, queries, keys, values):
    rows, width = 128, 2 * HEAD_DIM
    half = near.shape[0] // rows
    chunks = 2 * half
    lane = lax.broadcasted_iota(jnp.int32, (rows, width), 1)
    first = lane < HEAD_DIM
    one_lane = jnp.where(lane == 0, 1.0, 0.0).astype(jnp.bfloat16)
    for j in range(chunks):
        source = near if j < half else far
        at = (j % half) * rows
        here = slice(j * rows, (j + 1) * rows)
        low, high = slice(2 * j * rows, (2 * j + 1) * rows), slice((2 * j + 1) * rows, (2 * j + 2) * rows)
        q = source[at : at + rows, 0:width]
        zero = jnp.zeros_like(q)
        queries[low, 0:width] = jnp.where(first, q, zero)
        queries[high, 0:width] = jnp.where(first, zero, q)
        queries[low, width:] = one_lane
        queries[high, width:] = one_lane
        position = ids[j] * rows + lax.broadcasted_iota(jnp.int32, (rows, width), 0)
        masked = (position >= train[0]) & (lane == 0)
        keys[here, 0:width] = source[at : at + rows, width : 2 * width]
        keys[here, width:] = jnp.where(masked, MASKED, 0.0).astype(jnp.bfloat16)
        values[here, 0:width] = source[at : at + rows, 2 * width : 3 * width]
        values[here, width:] = jnp.ones((rows, width), jnp.bfloat16)

    for j in range(chunks):
        q = queries[2 * j * rows : (2 * j + 2) * rows, :]
        scores = lax.dot_general(
            q, keys[...], (((1,), (1,)), ((), ())), preferred_element_type=jnp.float32
        )
        top = jnp.max(scores, axis=1, keepdims=True)
        weights = jnp.exp2((scores - top) * (LOG2_E * HEAD_DIM**-0.5)).astype(jnp.bfloat16)
        mixed = jnp.dot(weights, values[...], preferred_element_type=jnp.float32)
        blended = mixed[:, :width] / mixed[:, width:]
        out[ids[j]] = jnp.where(first, blended[:rows], blended[rows:]).astype(jnp.bfloat16)


def attention(ids, train, near, far):
    chunks = ids.shape[0]
    rows, width = 128, 2 * HEAD_DIM
    vmem = pl.BlockSpec(memory_space=pltpu.VMEM)
    smem = pl.BlockSpec(memory_space=pltpu.SMEM)
    return pl.pallas_call(
        attention_kernel,
        out_shape=jax.ShapeDtypeStruct((chunks, rows, width), jnp.bfloat16),
        in_specs=[smem, smem, vmem, vmem],
        out_specs=vmem,
        scratch_shapes=[
            pltpu.VMEM((2 * chunks * rows, 2 * width), jnp.bfloat16),
            pltpu.VMEM((chunks * rows, 2 * width), jnp.bfloat16),
            pltpu.VMEM((chunks * rows, 2 * width), jnp.bfloat16),
        ],
        compiler_params=pltpu.CompilerParams(vmem_limit_bytes=20 * 2**20),
        name="attention",
    )(ids, train, near, far)


def local(
    inputs,
    selected,
    selection_gate,
    gate_weight,
    up_weight,
    down_weight,
    norm_gain,
    query_weight,
    key_weight,
    value_weight,
    train_count,
):
    exp_count = lax.axis_size("exp")
    ctx_count = lax.axis_size("ctx")
    exp_index = lax.axis_index("exp")
    ctx_index = lax.axis_index("ctx")
    row_count, model_width = inputs.shape
    experts = gate_weight.shape[0]
    group_take = selected.shape[1]
    table_rows = row_count * ctx_count
    head_width = model_width // ctx_count

    piece = jnp.concatenate(
        [
            lax.dynamic_slice_in_dim(w, ctx_index * head_width, head_width, 1)
            for w in (query_weight, key_weight, value_weight)
        ],
        axis=1,
    )
    own_block = exp_index * ctx_count + ctx_index
    taken = selected.reshape(exp_count, experts, group_take) - own_block * row_count
    mine = (taken >= 0) & (taken < row_count)
    lower = jnp.min(jnp.where(mine, taken, row_count), axis=2)
    upper = jnp.max(jnp.where(mine, taken, -1), axis=2)
    upper = jnp.where(upper > lower, upper, -1)
    picks = jnp.stack([lower, upper], axis=2)
    row_ids = jnp.arange(row_count, dtype=jnp.int32)
    owner_hit = (picks.reshape(-1, 1) == row_ids).astype(jnp.bfloat16)
    outgoing = jnp.dot(owner_hit, inputs, preferred_element_type=jnp.float32)
    outgoing = outgoing.astype(jnp.bfloat16).reshape(exp_count, -1, model_width)

    outgoing, piece = lax.optimization_barrier((outgoing, piece))
    quarter = gather_four(piece, exp_index // 4 % 4, 4)
    arrived = exchange(outgoing, "exp")
    arrived = arrived.reshape(-1, model_width)

    my_rows = lax.dynamic_slice_in_dim(selected, exp_index * experts, experts, 0)
    my_table = my_rows // table_rows
    lower_rows = (my_table[:, :, None] == my_table[:, None, :]) & (
        my_rows[:, None, :] < my_rows[:, :, None]
    )
    my_rank = jnp.sum(lower_rows.astype(jnp.int32), axis=2)
    expert_ids = jnp.arange(experts, dtype=jnp.int32)[:, None]
    my_place = ((my_table * experts + expert_ids) * MOST + my_rank).reshape(-1, 1)
    places = jnp.arange(exp_count * experts * MOST, dtype=jnp.int32)
    slot_hit = (my_place == places).astype(jnp.bfloat16)

    compact = jnp.dot(slot_hit, arrived, preferred_element_type=jnp.float32).astype(jnp.bfloat16)
    compact, quarter = lax.optimization_barrier((compact, quarter))
    layer = jnp.moveaxis(gather_four(quarter, exp_index % 4, 1), 0, 1)
    chosen = exchange(copies(compact, ctx_count), "ctx")
    partials = expert_parts(chosen, gate_weight, up_weight, down_weight)
    parts = exchange(partials, "ctx")
    expert_out = jnp.sum(parts.astype(jnp.float32), axis=0)
    weighted = (expert_out * selection_gate.reshape(-1, 1)).astype(jnp.bfloat16)
    reply = lax.dot_general(
        slot_hit, weighted, (((0,), (0,)), ((), ())), preferred_element_type=jnp.float32
    )
    reply = reply.astype(jnp.bfloat16).reshape(exp_count, -1, model_width)
    reply, layer = lax.optimization_barrier((reply, layer))
    weight_rows = gather_four(layer, exp_index // N_Z, N_Z).reshape(model_width, -1)
    returned = exchange(reply, "exp")
    returned = returned.reshape(-1, model_width)
    moe_sum = lax.dot_general(
        owner_hit, returned, (((0,), (0,)), ((), ())), preferred_element_type=jnp.float32
    )

    layer_out = (inputs.astype(jnp.float32) + moe_sum).astype(jnp.bfloat16)
    widened = layer_out.astype(jnp.float32)
    scale_row = lax.rsqrt(jnp.mean(widened * widened, axis=1, keepdims=True) + EPSILON)
    normed = (widened * scale_row * norm_gain).astype(jnp.bfloat16)

    near = jnp.concatenate(
        [normed, shift_chip(normed, 1), shift_chip(normed, -1), shift_chip(normed, 2)], axis=0
    )
    far = swap_core(near)
    chip, core = ctx_index // N_CORE, ctx_index % N_CORE
    steps = jnp.array([0, N_X - 1, 1, 2], jnp.int32)
    chips = (chip + steps) % N_X
    ids = jnp.concatenate([chips * N_CORE + core, chips * N_CORE + 1 - core])
    near_rows = jnp.dot(near, weight_rows, preferred_element_type=jnp.float32)
    far_rows = jnp.dot(far, weight_rows, preferred_element_type=jnp.float32)
    mixed = attention(
        ids, train_count, near_rows.astype(jnp.bfloat16), far_rows.astype(jnp.bfloat16)
    )
    by_heads = exchange(mixed, "ctx")
    context = jnp.moveaxis(by_heads, 0, 1).reshape(row_count, model_width)
    return (layer_out, context)


def solution(mesh):
    placed = (
        P(("exp", "ctx"), None),
        P(None, "ctx"),
        P("exp", "ctx"),
        P("exp", None, "ctx"),
        P("exp", None, "ctx"),
        P("exp", "ctx", None),
        P(),
        P("exp", None),
        P("exp", None),
        P("exp", None),
        P("exp"),
    )
    return jax.shard_map(
        local,
        mesh=mesh,
        in_specs=placed,
        out_specs=(P(("exp", "ctx"), None), P(("exp", "ctx"), None)),
        check_vma=False,
    )
```

```python
import jax
import jax.numpy as jnp
from jax import lax
from jax.experimental import pallas as pl
from jax.experimental.pallas import tpu as pltpu
from jax.sharding import PartitionSpec as P


HEAD_DIM = 64
EPSILON = 1e-06
MASKED = -1e30
LOG2_E = 1.4426950408889634
MOST = 2

N_Z = 16
N_X, N_CORE = 4, 2


def exchange(blocks, axis):
    return lax.all_to_all(blocks, axis, split_axis=0, concat_axis=0, tiled=True)


def shift(v, axis, move):
    count = lax.axis_size(axis)
    return lax.ppermute(v, axis, [(i, move(i)) for i in range(count)])


def shift_chip(v, step):
    return shift(v, "ctx", lambda i: (i // N_CORE + step) % N_X * N_CORE + i % N_CORE)


def swap_core(v):
    return shift(v, "ctx", lambda i: i ^ 1)


def gather_pair(v, index, stride):
    other = shift(v, "exp", lambda i: i ^ stride)
    turned = jnp.stack([other, v, other])
    return lax.dynamic_slice_in_dim(turned, 1 - index // stride % 2, 2, 0)


def gather_four(v, index, stride):
    pair = gather_pair(v, index, stride)
    four = gather_pair(pair, index, 2 * stride)
    return four.reshape(4, *v.shape)


def whole(memory, count):
    return [pl.BlockSpec(memory_space=memory) for _ in range(count)]


def small_kernel(body, outs, *arrays, scalars=0):
    return pl.pallas_call(
        body,
        out_shape=outs,
        in_specs=whole(pltpu.SMEM, scalars) + whole(pltpu.VMEM, len(arrays) - scalars),
        out_specs=pl.BlockSpec(memory_space=pltpu.VMEM),
        compiler_params=pltpu.CompilerParams(vmem_limit_bytes=8 * 2**20),
    )(*arrays)


def take_kernel(block, selected, inputs, out):
    row_count, width = inputs.shape
    taken = selected[...] - block[0] * row_count
    mine = (taken >= 0) & (taken < row_count)
    lower = jnp.min(jnp.where(mine, taken, row_count), axis=0, keepdims=True)
    upper = jnp.max(jnp.where(mine, taken, -1), axis=0, keepdims=True)
    upper = jnp.where(upper > lower, upper, -1)
    count = out.shape[0]
    experts = selected.shape[1]
    slot = lax.broadcasted_iota(jnp.int32, (count, experts), 0)
    expert = lax.broadcasted_iota(jnp.int32, (count, experts), 1)
    either = jnp.where(slot % 2 == 0, lower, upper)
    own = jnp.where(slot // 8 * 2 + slot % 4 // 2 == expert, either, 0)
    pick = jnp.dot(
        own.astype(jnp.float32).astype(jnp.bfloat16),
        jnp.ones((experts, row_count), jnp.bfloat16),
        preferred_element_type=jnp.float32,
    ).astype(jnp.int32)
    slot = lax.broadcasted_iota(jnp.int32, (count, row_count), 0)
    row = lax.broadcasted_iota(jnp.int32, (count, row_count), 1)
    hit = pick == row
    left = jnp.where(hit & (slot % 8 < 4), 1.0, 0.0).astype(jnp.bfloat16)
    right = jnp.where(hit & (slot % 8 >= 4), 1.0, 0.0).astype(jnp.bfloat16)
    half = width // 2
    out[...] = (
        jnp.dot(left, inputs[:, :half], preferred_element_type=jnp.float32)
        + jnp.dot(right, inputs[:, half:], preferred_element_type=jnp.float32)
    ).astype(out.dtype)


def fill_kernel(place, arrived, out):
    slots, half = place.shape[0], arrived.shape[1]
    source = lax.broadcasted_iota(jnp.int32, (slots, arrived.shape[0]), 1)
    for h in range(2):
        hit = jnp.where(source == place[...] + 4 * h, 1.0, 0.0).astype(jnp.bfloat16)
        rows = jnp.dot(hit, arrived[...], preferred_element_type=jnp.float32).astype(out.dtype)
        for c in range(out.shape[0]):
            out[c, :, h * half : (h + 1) * half] = rows


def reply_kernel(place, gate, parts, out):
    total = parts[0].astype(jnp.float32)
    for c in range(1, parts.shape[0]):
        total = total + parts[c].astype(jnp.float32)
    weighted = (total * gate[...]).astype(jnp.bfloat16)
    half = out.shape[1]
    target = lax.broadcasted_iota(jnp.int32, (out.shape[0], place.shape[1]), 0)
    left = jnp.where(target == place[...], 1.0, 0.0).astype(jnp.bfloat16)
    right = jnp.where(target == place[...] + 4, 1.0, 0.0).astype(jnp.bfloat16)
    out[...] = (
        jnp.dot(left, weighted[:, :half], preferred_element_type=jnp.float32)
        + jnp.dot(right, weighted[:, half:], preferred_element_type=jnp.float32)
    ).astype(out.dtype)


def join_kernel(pieces, out):
    width = pieces.shape[2]
    for c in range(pieces.shape[0]):
        out[:, c * width : (c + 1) * width] = pieces[c]


def expert_kernel(chosen, gate, up, down, out, down_here, sems):
    senders, _, width = chosen.shape
    experts = gate.shape[0]
    take = chosen.shape[1] // experts
    moves = [
        pltpu.make_async_copy(down.at[x], down_here.at[x], sems.at[x]) for x in range(experts)
    ]
    for move in moves:
        move.start()
    for x in range(experts):
        slots = slice(x * take, (x + 1) * take)
        rows = chosen[:, slots, :].reshape(senders * take, width)
        gate_part = jnp.dot(rows, gate[x], preferred_element_type=jnp.float32)
        up_part = jnp.dot(rows, up[x], preferred_element_type=jnp.float32)
        hidden = (gate_part / (1.0 + jnp.exp(-gate_part)) * up_part).astype(jnp.bfloat16)
        moves[x].wait()
        partial = jnp.dot(hidden, down_here[x], preferred_element_type=jnp.float32)
        out[:, slots, :] = partial.astype(jnp.bfloat16).reshape(senders, take, width)


def expert_parts(chosen, gate, up, down):
    vmem = pl.BlockSpec(memory_space=pltpu.VMEM)
    return pl.pallas_call(
        expert_kernel,
        out_shape=jax.ShapeDtypeStruct(chosen.shape, chosen.dtype),
        in_specs=[vmem, vmem, vmem, pl.BlockSpec(memory_space=pltpu.HBM)],
        out_specs=vmem,
        scratch_shapes=[
            pltpu.VMEM(down.shape, down.dtype),
            pltpu.SemaphoreType.DMA((down.shape[0],)),
        ],
        compiler_params=pltpu.CompilerParams(vmem_limit_bytes=12 * 2**20),
        name="experts",
    )(chosen, gate, up, pltpu.with_memory_space_constraint(down, pltpu.HBM))


def attention_kernel(ids, train, near, far, out, queries, keys, values):
    rows, width = 128, 2 * HEAD_DIM
    half = near.shape[0] // rows
    chunks = 2 * half
    lane = lax.broadcasted_iota(jnp.int32, (rows, width), 1)
    first = lane < HEAD_DIM
    one_lane = jnp.where(lane == 0, 1.0, 0.0).astype(jnp.bfloat16)
    for j in range(chunks):
        source = near if j < half else far
        at = (j % half) * rows
        here = slice(j * rows, (j + 1) * rows)
        low, high = slice(2 * j * rows, (2 * j + 1) * rows), slice((2 * j + 1) * rows, (2 * j + 2) * rows)
        q = source[at : at + rows, 0:width]
        zero = jnp.zeros_like(q)
        queries[low, 0:width] = jnp.where(first, q, zero)
        queries[high, 0:width] = jnp.where(first, zero, q)
        queries[low, width:] = one_lane
        queries[high, width:] = one_lane
        position = ids[j] * rows + lax.broadcasted_iota(jnp.int32, (rows, width), 0)
        masked = (position >= train[0]) & (lane == 0)
        keys[here, 0:width] = source[at : at + rows, width : 2 * width]
        keys[here, width:] = jnp.where(masked, MASKED, 0.0).astype(jnp.bfloat16)
        values[here, 0:width] = source[at : at + rows, 2 * width : 3 * width]
        values[here, width:] = jnp.ones((rows, width), jnp.bfloat16)

    for j in range(chunks):
        q = queries[2 * j * rows : (2 * j + 2) * rows, :]
        scores = lax.dot_general(
            q, keys[...], (((1,), (1,)), ((), ())), preferred_element_type=jnp.float32
        )
        top = jnp.max(scores, axis=1, keepdims=True)
        weights = jnp.exp2((scores - top) * (LOG2_E * HEAD_DIM**-0.5)).astype(jnp.bfloat16)
        mixed = jnp.dot(weights, values[...], preferred_element_type=jnp.float32)
        blended = mixed[:, :width] / mixed[:, width:]
        out[ids[j]] = jnp.where(first, blended[:rows], blended[rows:]).astype(jnp.bfloat16)


def attention(ids, train, near, far):
    chunks = ids.shape[0]
    rows, width = 128, 2 * HEAD_DIM
    vmem = pl.BlockSpec(memory_space=pltpu.VMEM)
    smem = pl.BlockSpec(memory_space=pltpu.SMEM)
    return pl.pallas_call(
        attention_kernel,
        out_shape=jax.ShapeDtypeStruct((chunks, rows, width), jnp.bfloat16),
        in_specs=[smem, smem, vmem, vmem],
        out_specs=vmem,
        scratch_shapes=[
            pltpu.VMEM((2 * chunks * rows, 2 * width), jnp.bfloat16),
            pltpu.VMEM((chunks * rows, 2 * width), jnp.bfloat16),
            pltpu.VMEM((chunks * rows, 2 * width), jnp.bfloat16),
        ],
        compiler_params=pltpu.CompilerParams(vmem_limit_bytes=20 * 2**20),
        name="attention",
    )(ids, train, near, far)


def local(
    inputs,
    selected,
    selection_gate,
    gate_weight,
    up_weight,
    down_weight,
    norm_gain,
    query_weight,
    key_weight,
    value_weight,
    train_count,
):
    exp_count = lax.axis_size("exp")
    ctx_count = lax.axis_size("ctx")
    exp_index = lax.axis_index("exp")
    ctx_index = lax.axis_index("ctx")
    row_count, model_width = inputs.shape
    experts = gate_weight.shape[0]
    group_take = selected.shape[1]
    table_rows = row_count * ctx_count
    head_width = model_width // ctx_count

    piece = jnp.concatenate(
        [
            lax.dynamic_slice_in_dim(w, ctx_index * head_width, head_width, 1)
            for w in (query_weight, key_weight, value_weight)
        ],
        axis=1,
    )
    own_block = exp_index * ctx_count + ctx_index
    half = model_width // 2
    sent = (exp_count, 2 * experts * MOST, half)
    flat = jax.ShapeDtypeStruct((sent[0] * sent[1], half), inputs.dtype)
    outgoing = small_kernel(take_kernel, flat, own_block.reshape(1), selected.T, inputs, scalars=1)
    arrived = exchange(outgoing.reshape(sent), "exp").reshape(flat.shape)
    quarter = gather_four(piece, exp_index, 4)
    arrived, quarter = lax.optimization_barrier((arrived, quarter))

    taken = selected.reshape(exp_count, experts, group_take) - own_block * row_count
    mine = (taken >= 0) & (taken < row_count)
    lower = jnp.min(jnp.where(mine, taken, row_count), axis=2)
    upper = jnp.max(jnp.where(mine, taken, -1), axis=2)
    upper = jnp.where(upper > lower, upper, -1)
    lower = jnp.where(lower < row_count, lower, -1)
    picks = jnp.stack([lower, upper], axis=2).reshape(exp_count, 1, experts * MOST)
    halves = jnp.arange(2, dtype=jnp.int32)[None, :, None] * row_count
    picks = jnp.where(picks < 0, -1, picks + halves).reshape(-1, 1)
    row_ids = jnp.arange(2 * row_count, dtype=jnp.int32)
    owner_hit = (picks == row_ids).astype(jnp.bfloat16)

    my_rows = lax.dynamic_slice_in_dim(selected, exp_index * experts, experts, 0)
    my_table = my_rows // table_rows
    lower_rows = (my_table[:, :, None] == my_table[:, None, :]) & (
        my_rows[:, None, :] < my_rows[:, :, None]
    )
    my_rank = jnp.sum(lower_rows.astype(jnp.int32), axis=2)
    expert_ids = jnp.arange(experts, dtype=jnp.int32)[:, None]
    my_place = (my_table * sent[1] + expert_ids * MOST + my_rank).reshape(-1)
    gates = selection_gate.reshape(-1, 1)

    chosen_shape = jax.ShapeDtypeStruct(
        (ctx_count, experts * group_take, model_width), inputs.dtype
    )
    compact = small_kernel(fill_kernel, chosen_shape, my_place.reshape(-1, 1), arrived)
    chosen = exchange(compact, "ctx")
    layer = jnp.moveaxis(gather_four(quarter, exp_index, 1), 0, 1)
    chosen, layer = lax.optimization_barrier((chosen, layer))
    partials = expert_parts(chosen, gate_weight, up_weight, down_weight)
    parts = exchange(partials, "ctx")
    reply = small_kernel(reply_kernel, flat, my_place.reshape(1, -1), gates, parts)
    returned = exchange(reply.reshape(sent), "exp").reshape(flat.shape)
    weight_rows = gather_four(layer, exp_index, N_Z).reshape(model_width, -1)
    returned, weight_rows = lax.optimization_barrier((returned, weight_rows))
    sums = lax.dot_general(
        owner_hit, returned, (((0,), (0,)), ((), ())), preferred_element_type=jnp.float32
    )
    moe_sum = jnp.concatenate([sums[:row_count], sums[row_count:]], axis=1)

    layer_out = (inputs.astype(jnp.float32) + moe_sum).astype(jnp.bfloat16)
    widened = layer_out.astype(jnp.float32)
    scale_row = lax.rsqrt(jnp.mean(widened * widened, axis=1, keepdims=True) + EPSILON)
    normed = (widened * scale_row * norm_gain).astype(jnp.bfloat16)

    near = jnp.concatenate(
        [normed, shift_chip(normed, 1), shift_chip(normed, -1), shift_chip(normed, 2)], axis=0
    )
    far = swap_core(near)
    chip, core = ctx_index // N_CORE, ctx_index % N_CORE
    steps = jnp.array([0, N_X - 1, 1, 2], jnp.int32)
    chips = (chip + steps) % N_X
    ids = jnp.concatenate([chips * N_CORE + core, chips * N_CORE + 1 - core])
    near_rows = jnp.dot(near, weight_rows, preferred_element_type=jnp.float32)
    far_rows = jnp.dot(far, weight_rows, preferred_element_type=jnp.float32)
    mixed = attention(
        ids, train_count, near_rows.astype(jnp.bfloat16), far_rows.astype(jnp.bfloat16)
    )
    by_heads = exchange(mixed, "ctx")
    context = small_kernel(join_kernel, jax.ShapeDtypeStruct(inputs.shape, inputs.dtype), by_heads)
    return (layer_out, context)


def solution(mesh):
    placed = (
        P(("exp", "ctx"), None),
        P(None, "ctx"),
        P("exp", "ctx"),
        P("exp", None, "ctx"),
        P("exp", None, "ctx"),
        P("exp", "ctx", None),
        P(),
        P("exp", None),
        P("exp", None),
        P("exp", None),
        P("exp"),
    )
    return jax.shard_map(
        local,
        mesh=mesh,
        in_specs=placed,
        out_specs=(P(("exp", "ctx"), None), P(("exp", "ctx"), None)),
        check_vma=False,
    )
```

```python
import jax
import jax.numpy as jnp
from jax import lax
from jax.experimental import pallas as pl
from jax.experimental.pallas import tpu as pltpu
from jax.sharding import PartitionSpec as P


HEAD_DIM = 64
EPSILON = 1e-06
MASKED = -1e30
LOG2_E = 1.4426950408889634
MOST = 2

N_Z = 16
N_X, N_CORE = 4, 2


def exchange(blocks, axis):
    return lax.all_to_all(blocks, axis, split_axis=0, concat_axis=0, tiled=True)


def shift(v, axis, move):
    count = lax.axis_size(axis)
    return lax.ppermute(v, axis, [(i, move(i)) for i in range(count)])


def shift_chip(v, step):
    return shift(v, "ctx", lambda i: (i // N_CORE + step) % N_X * N_CORE + i % N_CORE)


def swap_core(v):
    return shift(v, "ctx", lambda i: i ^ 1)


def gather_four(v, digit, stride):
    def move(step):
        return lambda i: i + ((i // stride + step) % 4 - i // stride % 4) * stride

    others = []
    for step in (1, 2, 3):
        others.append(shift(v, "exp", move(step)))
    one, two, three = others
    turned = jnp.stack([three, two, one, v, three, two, one])
    return lax.dynamic_slice_in_dim(turned, 3 - digit, 4, 0)


def whole(memory, count):
    return [pl.BlockSpec(memory_space=memory) for _ in range(count)]


def small_kernel(body, outs, *arrays, scalars=0):
    return pl.pallas_call(
        body,
        out_shape=outs,
        in_specs=whole(pltpu.SMEM, scalars) + whole(pltpu.VMEM, len(arrays) - scalars),
        out_specs=pl.BlockSpec(memory_space=pltpu.VMEM),
        compiler_params=pltpu.CompilerParams(vmem_limit_bytes=8 * 2**20),
    )(*arrays)


def in_hbm(v):
    return pltpu.with_memory_space_constraint(v, pltpu.HBM)


def take_kernel(block, selected, inputs, out):
    row_count, width = inputs.shape
    taken = selected[...] - block[0] * row_count
    mine = (taken >= 0) & (taken < row_count)
    lower = jnp.min(jnp.where(mine, taken, row_count), axis=0, keepdims=True)
    upper = jnp.max(jnp.where(mine, taken, -1), axis=0, keepdims=True)
    upper = jnp.where(upper > lower, upper, -1)
    count = out.shape[0]
    experts = selected.shape[1]
    slot = lax.broadcasted_iota(jnp.int32, (count, experts), 0)
    expert = lax.broadcasted_iota(jnp.int32, (count, experts), 1)
    either = jnp.where(slot % 2 == 0, lower, upper)
    own = jnp.where(slot // 8 * 2 + slot % 4 // 2 == expert, either, 0)
    pick = jnp.dot(
        own.astype(jnp.float32).astype(jnp.bfloat16),
        jnp.ones((experts, row_count), jnp.bfloat16),
        preferred_element_type=jnp.float32,
    ).astype(jnp.int32)
    slot = lax.broadcasted_iota(jnp.int32, (count, row_count), 0)
    row = lax.broadcasted_iota(jnp.int32, (count, row_count), 1)
    hit = pick == row
    left = jnp.where(hit & (slot % 8 < 4), 1.0, 0.0).astype(jnp.bfloat16)
    right = jnp.where(hit & (slot % 8 >= 4), 1.0, 0.0).astype(jnp.bfloat16)
    half = width // 2
    out[...] = (
        jnp.dot(left, inputs[:, :half], preferred_element_type=jnp.float32)
        + jnp.dot(right, inputs[:, half:], preferred_element_type=jnp.float32)
    ).astype(out.dtype)


def fill_kernel(place, arrived, out):
    slots, half = place.shape[0], arrived.shape[1]
    source = lax.broadcasted_iota(jnp.int32, (slots, arrived.shape[0]), 1)
    for h in range(2):
        hit = jnp.where(source == place[...] + 4 * h, 1.0, 0.0).astype(jnp.bfloat16)
        rows = jnp.dot(hit, arrived[...], preferred_element_type=jnp.float32).astype(out.dtype)
        for c in range(out.shape[0]):
            out[c, :, h * half : (h + 1) * half] = rows


def reply_kernel(place, gate, parts, out):
    total = parts[0].astype(jnp.float32)
    for c in range(1, parts.shape[0]):
        total = total + parts[c].astype(jnp.float32)
    weighted = (total * gate[...]).astype(jnp.bfloat16)
    half = out.shape[1]
    target = lax.broadcasted_iota(jnp.int32, (out.shape[0], place.shape[1]), 0)
    left = jnp.where(target == place[...], 1.0, 0.0).astype(jnp.bfloat16)
    right = jnp.where(target == place[...] + 4, 1.0, 0.0).astype(jnp.bfloat16)
    out[...] = (
        jnp.dot(left, weighted[:, :half], preferred_element_type=jnp.float32)
        + jnp.dot(right, weighted[:, half:], preferred_element_type=jnp.float32)
    ).astype(out.dtype)


def join_kernel(pieces, out):
    width = pieces.shape[2]
    for c in range(pieces.shape[0]):
        out[:, c * width : (c + 1) * width] = pieces[c]


def expert_kernel(chosen, gate, up, down, out, down_here, sems):
    senders, _, width = chosen.shape
    experts = gate.shape[0]
    take = chosen.shape[1] // experts
    moves = [
        pltpu.make_async_copy(down.at[x], down_here.at[x], sems.at[x]) for x in range(experts)
    ]
    for move in moves:
        move.start()
    for x in range(experts):
        slots = slice(x * take, (x + 1) * take)
        rows = chosen[:, slots, :].reshape(senders * take, width)
        gate_part = jnp.dot(rows, gate[x], preferred_element_type=jnp.float32)
        up_part = jnp.dot(rows, up[x], preferred_element_type=jnp.float32)
        hidden = (gate_part / (1.0 + jnp.exp(-gate_part)) * up_part).astype(jnp.bfloat16)
        moves[x].wait()
        partial = jnp.dot(hidden, down_here[x], preferred_element_type=jnp.float32)
        out[:, slots, :] = partial.astype(jnp.bfloat16).reshape(senders, take, width)


def expert_parts(chosen, gate, up, down):
    vmem = pl.BlockSpec(memory_space=pltpu.VMEM)
    return pl.pallas_call(
        expert_kernel,
        out_shape=jax.ShapeDtypeStruct(chosen.shape, chosen.dtype),
        in_specs=[vmem, vmem, vmem, pl.BlockSpec(memory_space=pltpu.HBM)],
        out_specs=vmem,
        scratch_shapes=[
            pltpu.VMEM(down.shape, down.dtype),
            pltpu.SemaphoreType.DMA((down.shape[0],)),
        ],
        compiler_params=pltpu.CompilerParams(vmem_limit_bytes=12 * 2**20),
        name="experts",
    )(chosen, gate, up, in_hbm(down))


def attention_kernel(ids, train, near, far, out, queries, keys, values):
    rows, width = 128, 2 * HEAD_DIM
    half = near.shape[0] // rows
    chunks = 2 * half
    lane = lax.broadcasted_iota(jnp.int32, (rows, width), 1)
    first = lane < HEAD_DIM
    one_lane = jnp.where(lane == 0, 1.0, 0.0).astype(jnp.bfloat16)
    for j in range(chunks):
        source = near if j < half else far
        at = (j % half) * rows
        here = slice(j * rows, (j + 1) * rows)
        low, high = slice(2 * j * rows, (2 * j + 1) * rows), slice((2 * j + 1) * rows, (2 * j + 2) * rows)
        q = source[at : at + rows, 0:width]
        zero = jnp.zeros_like(q)
        queries[low, 0:width] = jnp.where(first, q, zero)
        queries[high, 0:width] = jnp.where(first, zero, q)
        queries[low, width:] = one_lane
        queries[high, width:] = one_lane
        position = ids[j] * rows + lax.broadcasted_iota(jnp.int32, (rows, width), 0)
        masked = (position >= train[0]) & (lane == 0)
        keys[here, 0:width] = source[at : at + rows, width : 2 * width]
        keys[here, width:] = jnp.where(masked, MASKED, 0.0).astype(jnp.bfloat16)
        values[here, 0:width] = source[at : at + rows, 2 * width : 3 * width]
        values[here, width:] = jnp.ones((rows, width), jnp.bfloat16)

    for j in range(chunks):
        q = queries[2 * j * rows : (2 * j + 2) * rows, :]
        scores = lax.dot_general(
            q, keys[...], (((1,), (1,)), ((), ())), preferred_element_type=jnp.float32
        )
        top = jnp.max(scores, axis=1, keepdims=True)
        weights = jnp.exp2((scores - top) * (LOG2_E * HEAD_DIM**-0.5)).astype(jnp.bfloat16)
        mixed = jnp.dot(weights, values[...], preferred_element_type=jnp.float32)
        blended = mixed[:, :width] / mixed[:, width:]
        out[ids[j]] = jnp.where(first, blended[:rows], blended[rows:]).astype(jnp.bfloat16)


def attention(ids, train, near, far):
    chunks = ids.shape[0]
    rows, width = 128, 2 * HEAD_DIM
    vmem = pl.BlockSpec(memory_space=pltpu.VMEM)
    smem = pl.BlockSpec(memory_space=pltpu.SMEM)
    return pl.pallas_call(
        attention_kernel,
        out_shape=jax.ShapeDtypeStruct((chunks, rows, width), jnp.bfloat16),
        in_specs=[smem, smem, vmem, vmem],
        out_specs=vmem,
        scratch_shapes=[
            pltpu.VMEM((2 * chunks * rows, 2 * width), jnp.bfloat16),
            pltpu.VMEM((chunks * rows, 2 * width), jnp.bfloat16),
            pltpu.VMEM((chunks * rows, 2 * width), jnp.bfloat16),
        ],
        compiler_params=pltpu.CompilerParams(vmem_limit_bytes=20 * 2**20),
        name="attention",
    )(ids, train, near, far)


def local(
    inputs,
    selected,
    selection_gate,
    gate_weight,
    up_weight,
    down_weight,
    norm_gain,
    query_weight,
    key_weight,
    value_weight,
    train_count,
):
    exp_count = lax.axis_size("exp")
    ctx_count = lax.axis_size("ctx")
    exp_index = lax.axis_index("exp")
    ctx_index = lax.axis_index("ctx")
    row_count, model_width = inputs.shape
    experts = gate_weight.shape[0]
    group_take = selected.shape[1]
    table_rows = row_count * ctx_count
    head_width = model_width // ctx_count

    piece = jnp.concatenate(
        [
            lax.dynamic_slice_in_dim(w, ctx_index * head_width, head_width, 1)
            for w in (query_weight, key_weight, value_weight)
        ],
        axis=1,
    )
    own_block = exp_index * ctx_count + ctx_index
    half = model_width // 2
    sent = (exp_count, 2 * experts * MOST, half)
    flat = jax.ShapeDtypeStruct((sent[0] * sent[1], half), inputs.dtype)
    outgoing = small_kernel(
        take_kernel, flat, own_block.reshape(1), in_hbm(selected.T), in_hbm(inputs), scalars=1
    )
    arrived = exchange(outgoing.reshape(sent), "exp").reshape(flat.shape)
    quarter = gather_four(piece, exp_index // 4 % 4, 4)

    taken = selected.reshape(exp_count, experts, group_take) - own_block * row_count
    mine = (taken >= 0) & (taken < row_count)
    lower = jnp.min(jnp.where(mine, taken, row_count), axis=2)
    upper = jnp.max(jnp.where(mine, taken, -1), axis=2)
    upper = jnp.where(upper > lower, upper, -1)
    lower = jnp.where(lower < row_count, lower, -1)
    picks = jnp.stack([lower, upper], axis=2).reshape(exp_count, 1, experts * MOST)
    halves = jnp.arange(2, dtype=jnp.int32)[None, :, None] * row_count
    picks = jnp.where(picks < 0, -1, picks + halves).reshape(-1, 1)
    row_ids = jnp.arange(2 * row_count, dtype=jnp.int32)
    owner_hit = (picks == row_ids).astype(jnp.bfloat16)

    my_rows = lax.dynamic_slice_in_dim(selected, exp_index * experts, experts, 0)
    my_table = my_rows // table_rows
    lower_rows = (my_table[:, :, None] == my_table[:, None, :]) & (
        my_rows[:, None, :] < my_rows[:, :, None]
    )
    my_rank = jnp.sum(lower_rows.astype(jnp.int32), axis=2)
    expert_ids = jnp.arange(experts, dtype=jnp.int32)[:, None]
    my_place = (my_table * sent[1] + expert_ids * MOST + my_rank).reshape(-1)
    gates = selection_gate.reshape(-1, 1)

    chosen_shape = jax.ShapeDtypeStruct(
        (ctx_count, experts * group_take, model_width), inputs.dtype
    )
    compact = small_kernel(fill_kernel, chosen_shape, my_place.reshape(-1, 1), arrived)
    chosen = exchange(compact, "ctx")
    layer = jnp.moveaxis(gather_four(quarter, exp_index % 4, 1), 0, 1)
    partials = expert_parts(chosen, gate_weight, up_weight, down_weight)
    parts = exchange(partials, "ctx")
    reply = small_kernel(reply_kernel, flat, my_place.reshape(1, -1), gates, parts)
    reply, layer = lax.optimization_barrier((reply, layer))
    returned = exchange(reply.reshape(sent), "exp").reshape(flat.shape)
    weight_rows = gather_four(layer, exp_index // N_Z, N_Z).reshape(model_width, -1)
    sums = lax.dot_general(
        owner_hit, returned, (((0,), (0,)), ((), ())), preferred_element_type=jnp.float32
    )
    moe_sum = jnp.concatenate([sums[:row_count], sums[row_count:]], axis=1)

    layer_out = (inputs.astype(jnp.float32) + moe_sum).astype(jnp.bfloat16)
    widened = layer_out.astype(jnp.float32)
    scale_row = lax.rsqrt(jnp.mean(widened * widened, axis=1, keepdims=True) + EPSILON)
    normed = (widened * scale_row * norm_gain).astype(jnp.bfloat16)

    near = jnp.concatenate(
        [normed, shift_chip(normed, 1), shift_chip(normed, -1), shift_chip(normed, 2)], axis=0
    )
    far = swap_core(near)
    chip, core = ctx_index // N_CORE, ctx_index % N_CORE
    steps = jnp.array([0, N_X - 1, 1, 2], jnp.int32)
    chips = (chip + steps) % N_X
    ids = jnp.concatenate([chips * N_CORE + core, chips * N_CORE + 1 - core])
    near_rows = jnp.dot(near, weight_rows, preferred_element_type=jnp.float32)
    far_rows = jnp.dot(far, weight_rows, preferred_element_type=jnp.float32)
    mixed = attention(
        ids, train_count, near_rows.astype(jnp.bfloat16), far_rows.astype(jnp.bfloat16)
    )
    by_heads = exchange(mixed, "ctx")
    context = small_kernel(join_kernel, jax.ShapeDtypeStruct(inputs.shape, inputs.dtype), by_heads)
    return (layer_out, context)


def solution(mesh):
    placed = (
        P(("exp", "ctx"), None),
        P(None, "ctx"),
        P("exp", "ctx"),
        P("exp", None, "ctx"),
        P("exp", None, "ctx"),
        P("exp", "ctx", None),
        P(),
        P("exp", None),
        P("exp", None),
        P("exp", None),
        P("exp"),
    )
    return jax.shard_map(
        local,
        mesh=mesh,
        in_specs=placed,
        out_specs=(P(("exp", "ctx"), None), P(("exp", "ctx"), None)),
        check_vma=False,
    )
```

```python
import jax
import jax.numpy as jnp
from jax import lax
from jax.experimental import pallas as pl
from jax.experimental.pallas import tpu as pltpu
from jax.sharding import PartitionSpec as P


HEAD_DIM = 64
EPSILON = 1e-06
MASKED = -1e30
LOG2_E = 1.4426950408889634
MOST = 2

N_Z = 16
N_X, N_CORE = 4, 2


def exchange(blocks, axis):
    return lax.all_to_all(blocks, axis, split_axis=0, concat_axis=0, tiled=True)


def shift(v, axis, move):
    count = lax.axis_size(axis)
    return lax.ppermute(v, axis, [(i, move(i)) for i in range(count)])


def shift_chip(v, step):
    return shift(v, "ctx", lambda i: (i // N_CORE + step) % N_X * N_CORE + i % N_CORE)


def swap_core(v):
    return shift(v, "ctx", lambda i: i ^ 1)


def gather_four(v, digit, stride, after=None):
    def move(step):
        return lambda i: i + ((i // stride + step) % 4 - i // stride % 4) * stride

    others = []
    for step in (1, 2, 3):
        others.append(shift(v, "exp", move(step)))
    if after is not None:
        *others, _ = lax.optimization_barrier((*others, after()))
    one, two, three = others
    turned = jnp.stack([three, two, one, v, three, two, one])
    return lax.dynamic_slice_in_dim(turned, 3 - digit, 4, 0)


def whole(memory, count):
    return [pl.BlockSpec(memory_space=memory) for _ in range(count)]


def small_kernel(body, outs, *arrays, scalars=0):
    return pl.pallas_call(
        body,
        out_shape=outs,
        in_specs=whole(pltpu.SMEM, scalars) + whole(pltpu.VMEM, len(arrays) - scalars),
        out_specs=pl.BlockSpec(memory_space=pltpu.VMEM),
        compiler_params=pltpu.CompilerParams(vmem_limit_bytes=8 * 2**20),
    )(*arrays)


def in_hbm(v):
    return pltpu.with_memory_space_constraint(v, pltpu.HBM)


def take_kernel(block, selected, inputs, out):
    row_count, width = inputs.shape
    taken = selected[...] - block[0] * row_count
    mine = (taken >= 0) & (taken < row_count)
    lower = jnp.min(jnp.where(mine, taken, row_count), axis=0, keepdims=True)
    upper = jnp.max(jnp.where(mine, taken, -1), axis=0, keepdims=True)
    upper = jnp.where(upper > lower, upper, -1)
    count = out.shape[0]
    experts = selected.shape[1]
    slot = lax.broadcasted_iota(jnp.int32, (count, experts), 0)
    expert = lax.broadcasted_iota(jnp.int32, (count, experts), 1)
    either = jnp.where(slot % 2 == 0, lower, upper)
    own = jnp.where(slot // 8 * 2 + slot % 4 // 2 == expert, either, 0)
    pick = jnp.dot(
        own.astype(jnp.float32).astype(jnp.bfloat16),
        jnp.ones((experts, row_count), jnp.bfloat16),
        preferred_element_type=jnp.float32,
    ).astype(jnp.int32)
    slot = lax.broadcasted_iota(jnp.int32, (count, row_count), 0)
    row = lax.broadcasted_iota(jnp.int32, (count, row_count), 1)
    hit = pick == row
    left = jnp.where(hit & (slot % 8 < 4), 1.0, 0.0).astype(jnp.bfloat16)
    right = jnp.where(hit & (slot % 8 >= 4), 1.0, 0.0).astype(jnp.bfloat16)
    half = width // 2
    out[...] = (
        jnp.dot(left, inputs[:, :half], preferred_element_type=jnp.float32)
        + jnp.dot(right, inputs[:, half:], preferred_element_type=jnp.float32)
    ).astype(out.dtype)


def fill_kernel(place, arrived, out):
    slots, half = place.shape[0], arrived.shape[1]
    source = lax.broadcasted_iota(jnp.int32, (slots, arrived.shape[0]), 1)
    for h in range(2):
        hit = jnp.where(source == place[...] + 4 * h, 1.0, 0.0).astype(jnp.bfloat16)
        rows = jnp.dot(hit, arrived[...], preferred_element_type=jnp.float32).astype(out.dtype)
        for c in range(out.shape[0]):
            out[c, :, h * half : (h + 1) * half] = rows


def reply_kernel(place, gate, parts, out):
    total = parts[0].astype(jnp.float32)
    for c in range(1, parts.shape[0]):
        total = total + parts[c].astype(jnp.float32)
    weighted = (total * gate[...]).astype(jnp.bfloat16)
    half = out.shape[1]
    target = lax.broadcasted_iota(jnp.int32, (out.shape[0], place.shape[1]), 0)
    left = jnp.where(target == place[...], 1.0, 0.0).astype(jnp.bfloat16)
    right = jnp.where(target == place[...] + 4, 1.0, 0.0).astype(jnp.bfloat16)
    out[...] = (
        jnp.dot(left, weighted[:, :half], preferred_element_type=jnp.float32)
        + jnp.dot(right, weighted[:, half:], preferred_element_type=jnp.float32)
    ).astype(out.dtype)


def join_kernel(pieces, out):
    width = pieces.shape[2]
    for c in range(pieces.shape[0]):
        out[:, c * width : (c + 1) * width] = pieces[c]


def expert_kernel(chosen, gate, up, down, out, down_here, sems):
    senders, _, width = chosen.shape
    experts = gate.shape[0]
    take = chosen.shape[1] // experts
    moves = [
        pltpu.make_async_copy(down.at[x], down_here.at[x], sems.at[x]) for x in range(experts)
    ]
    for move in moves:
        move.start()
    for x in range(experts):
        slots = slice(x * take, (x + 1) * take)
        rows = chosen[:, slots, :].reshape(senders * take, width)
        gate_part = jnp.dot(rows, gate[x], preferred_element_type=jnp.float32)
        up_part = jnp.dot(rows, up[x], preferred_element_type=jnp.float32)
        hidden = (gate_part / (1.0 + jnp.exp(-gate_part)) * up_part).astype(jnp.bfloat16)
        moves[x].wait()
        partial = jnp.dot(hidden, down_here[x], preferred_element_type=jnp.float32)
        out[:, slots, :] = partial.astype(jnp.bfloat16).reshape(senders, take, width)


def expert_parts(chosen, gate, up, down):
    vmem = pl.BlockSpec(memory_space=pltpu.VMEM)
    return pl.pallas_call(
        expert_kernel,
        out_shape=jax.ShapeDtypeStruct(chosen.shape, chosen.dtype),
        in_specs=[vmem, vmem, vmem, pl.BlockSpec(memory_space=pltpu.HBM)],
        out_specs=vmem,
        scratch_shapes=[
            pltpu.VMEM(down.shape, down.dtype),
            pltpu.SemaphoreType.DMA((down.shape[0],)),
        ],
        compiler_params=pltpu.CompilerParams(vmem_limit_bytes=12 * 2**20),
        name="experts",
    )(chosen, gate, up, in_hbm(down))


def attention_kernel(ids, train, *refs):
    *sources, out, queries, keys, values = refs
    rows, width = 128, 2 * HEAD_DIM
    chunks = out.shape[0]
    places = [(source, at) for source in sources for at in range(0, source.shape[0], rows)]
    lane = lax.broadcasted_iota(jnp.int32, (rows, width), 1)
    first = lane < HEAD_DIM
    one_lane = jnp.where(lane == 0, 1.0, 0.0).astype(jnp.bfloat16)
    for j in range(chunks):
        source, at = places[j]
        here = slice(j * rows, (j + 1) * rows)
        low, high = slice(2 * j * rows, (2 * j + 1) * rows), slice((2 * j + 1) * rows, (2 * j + 2) * rows)
        q = source[at : at + rows, 0:width]
        zero = jnp.zeros_like(q)
        queries[low, 0:width] = jnp.where(first, q, zero)
        queries[high, 0:width] = jnp.where(first, zero, q)
        queries[low, width:] = one_lane
        queries[high, width:] = one_lane
        position = ids[j] * rows + lax.broadcasted_iota(jnp.int32, (rows, width), 0)
        masked = (position >= train[0]) & (lane == 0)
        keys[here, 0:width] = source[at : at + rows, width : 2 * width]
        keys[here, width:] = jnp.where(masked, MASKED, 0.0).astype(jnp.bfloat16)
        values[here, 0:width] = source[at : at + rows, 2 * width : 3 * width]
        values[here, width:] = jnp.ones((rows, width), jnp.bfloat16)

    for j in range(chunks):
        q = queries[2 * j * rows : (2 * j + 2) * rows, :]
        scores = lax.dot_general(
            q, keys[...], (((1,), (1,)), ((), ())), preferred_element_type=jnp.float32
        )
        top = jnp.max(scores, axis=1, keepdims=True)
        weights = jnp.exp2((scores - top) * (LOG2_E * HEAD_DIM**-0.5)).astype(jnp.bfloat16)
        mixed = jnp.dot(weights, values[...], preferred_element_type=jnp.float32)
        blended = mixed[:, :width] / mixed[:, width:]
        out[ids[j]] = jnp.where(first, blended[:rows], blended[rows:]).astype(jnp.bfloat16)


def attention(ids, train, sources):
    chunks = ids.shape[0]
    rows, width = 128, 2 * HEAD_DIM
    vmem = pl.BlockSpec(memory_space=pltpu.VMEM)
    smem = pl.BlockSpec(memory_space=pltpu.SMEM)
    return pl.pallas_call(
        attention_kernel,
        out_shape=jax.ShapeDtypeStruct((chunks, rows, width), jnp.bfloat16),
        in_specs=[smem, smem] + [vmem] * len(sources),
        out_specs=vmem,
        scratch_shapes=[
            pltpu.VMEM((2 * chunks * rows, 2 * width), jnp.bfloat16),
            pltpu.VMEM((chunks * rows, 2 * width), jnp.bfloat16),
            pltpu.VMEM((chunks * rows, 2 * width), jnp.bfloat16),
        ],
        compiler_params=pltpu.CompilerParams(vmem_limit_bytes=20 * 2**20),
        name="attention",
    )(ids, train, *sources)


def local(
    inputs,
    selected,
    selection_gate,
    gate_weight,
    up_weight,
    down_weight,
    norm_gain,
    query_weight,
    key_weight,
    value_weight,
    train_count,
):
    exp_count = lax.axis_size("exp")
    ctx_count = lax.axis_size("ctx")
    exp_index = lax.axis_index("exp")
    ctx_index = lax.axis_index("ctx")
    row_count, model_width = inputs.shape
    experts = gate_weight.shape[0]
    group_take = selected.shape[1]
    table_rows = row_count * ctx_count
    head_width = model_width // ctx_count

    piece = jnp.concatenate(
        [
            lax.dynamic_slice_in_dim(w, ctx_index * head_width, head_width, 1)
            for w in (query_weight, key_weight, value_weight)
        ],
        axis=1,
    )
    own_block = exp_index * ctx_count + ctx_index
    half = model_width // 2
    sent = (exp_count, 2 * experts * MOST, half)
    flat = jax.ShapeDtypeStruct((sent[0] * sent[1], half), inputs.dtype)
    outgoing = small_kernel(
        take_kernel, flat, own_block.reshape(1), in_hbm(selected.T), in_hbm(inputs), scalars=1
    )
    arrived = exchange(outgoing.reshape(sent), "exp").reshape(flat.shape)
    taken = selected.reshape(exp_count, experts, group_take) - own_block * row_count
    mine = (taken >= 0) & (taken < row_count)
    lower = jnp.min(jnp.where(mine, taken, row_count), axis=2)
    upper = jnp.max(jnp.where(mine, taken, -1), axis=2)
    upper = jnp.where(upper > lower, upper, -1)
    lower = jnp.where(lower < row_count, lower, -1)
    picks = jnp.stack([lower, upper], axis=2).reshape(exp_count, 1, experts * MOST)
    halves = jnp.arange(2, dtype=jnp.int32)[None, :, None] * row_count
    picks = jnp.where(picks < 0, -1, picks + halves).reshape(-1, 1)
    row_ids = jnp.arange(2 * row_count, dtype=jnp.int32)
    owner_hit = (picks == row_ids).astype(jnp.bfloat16)

    my_rows = lax.dynamic_slice_in_dim(selected, exp_index * experts, experts, 0)
    my_table = my_rows // table_rows
    lower_rows = (my_table[:, :, None] == my_table[:, None, :]) & (
        my_rows[:, None, :] < my_rows[:, :, None]
    )
    my_rank = jnp.sum(lower_rows.astype(jnp.int32), axis=2)
    expert_ids = jnp.arange(experts, dtype=jnp.int32)[:, None]
    my_place = (my_table * sent[1] + expert_ids * MOST + my_rank).reshape(-1)
    gates = selection_gate.reshape(-1, 1)

    chosen_shape = jax.ShapeDtypeStruct(
        (ctx_count, experts * group_take, model_width), inputs.dtype
    )
    compact = small_kernel(fill_kernel, chosen_shape, my_place.reshape(-1, 1), arrived)
    chosen = exchange(compact, "ctx")
    quarter = gather_four(piece, exp_index // 4 % 4, 4, lambda: compact)
    layer = jnp.moveaxis(gather_four(quarter, exp_index % 4, 1), 0, 1)
    partials = expert_parts(chosen, gate_weight, up_weight, down_weight)
    parts = exchange(partials, "ctx")
    reply = small_kernel(reply_kernel, flat, my_place.reshape(1, -1), gates, parts)
    reply, layer = lax.optimization_barrier((reply, layer))
    returned = exchange(reply.reshape(sent), "exp").reshape(flat.shape)
    weight_rows = gather_four(layer, exp_index // N_Z, N_Z).reshape(model_width, -1)
    sums = lax.dot_general(
        owner_hit, returned, (((0,), (0,)), ((), ())), preferred_element_type=jnp.float32
    )
    moe_sum = jnp.concatenate([sums[:row_count], sums[row_count:]], axis=1)

    layer_out = (inputs.astype(jnp.float32) + moe_sum).astype(jnp.bfloat16)
    widened = layer_out.astype(jnp.float32)
    scale_row = lax.rsqrt(jnp.mean(widened * widened, axis=1, keepdims=True) + EPSILON)
    normed = (widened * scale_row * norm_gain).astype(jnp.bfloat16)

    arrived = []
    for step in (1, -1, 2):
        arrived.append(shift_chip(normed, step))
    near = [normed, jnp.concatenate(arrived[:2], axis=0), arrived[2]]
    far = []
    for chunk in near:
        far.append(swap_core(chunk))
    chip, core = ctx_index // N_CORE, ctx_index % N_CORE
    steps = jnp.array([0, N_X - 1, 1, 2], jnp.int32)
    chips = (chip + steps) % N_X
    ids = jnp.concatenate([chips * N_CORE + core, chips * N_CORE + 1 - core])
    projected = [
        jnp.dot(rows, weight_rows, preferred_element_type=jnp.float32).astype(jnp.bfloat16)
        for rows in near + far
    ]
    mixed = attention(ids, train_count, projected)
    by_heads = exchange(mixed, "ctx")
    context = small_kernel(join_kernel, jax.ShapeDtypeStruct(inputs.shape, inputs.dtype), by_heads)
    return (layer_out, context)


def solution(mesh):
    placed = (
        P(("exp", "ctx"), None),
        P(None, "ctx"),
        P("exp", "ctx"),
        P("exp", None, "ctx"),
        P("exp", None, "ctx"),
        P("exp", "ctx", None),
        P(),
        P("exp", None),
        P("exp", None),
        P("exp", None),
        P("exp"),
    )
    return jax.shard_map(
        local,
        mesh=mesh,
        in_specs=placed,
        out_specs=(P(("exp", "ctx"), None), P(("exp", "ctx"), None)),
        check_vma=False,
    )
```

```python
import jax
import jax.numpy as jnp
from jax import lax
from jax.experimental import pallas as pl
from jax.experimental.pallas import tpu as pltpu
from jax.sharding import PartitionSpec as P


HEAD_DIM = 64
EPSILON = 1e-06
MASKED = -1e30
LOG2_E = 1.4426950408889634
MOST = 2

N_Z = 16
N_X, N_CORE = 4, 2


def exchange(blocks, axis):
    return lax.all_to_all(blocks, axis, split_axis=0, concat_axis=0, tiled=True)


def shift(v, axis, move):
    count = lax.axis_size(axis)
    return lax.ppermute(v, axis, [(i, move(i)) for i in range(count)])


def shift_chip(v, step):
    return shift(v, "ctx", lambda i: (i // N_CORE + step) % N_X * N_CORE + i % N_CORE)


def swap_core(v):
    return shift(v, "ctx", lambda i: i ^ 1)


def gather_four(v, digit, stride, after=None):
    def move(step):
        return lambda i: i + ((i // stride + step) % 4 - i // stride % 4) * stride

    others = []
    for step in (1, 2, 3):
        others.append(shift(v, "exp", move(step)))
    if after is not None:
        *others, _ = lax.optimization_barrier((*others, after))
    one, two, three = others
    turned = jnp.stack([three, two, one, v, three, two, one])
    return lax.dynamic_slice_in_dim(turned, 3 - digit, 4, 0)


def whole(memory, count):
    return [pl.BlockSpec(memory_space=memory) for _ in range(count)]


def small_kernel(body, outs, *arrays, scalars=0):
    return pl.pallas_call(
        body,
        out_shape=outs,
        in_specs=whole(pltpu.SMEM, scalars) + whole(pltpu.VMEM, len(arrays) - scalars),
        out_specs=pl.BlockSpec(memory_space=pltpu.VMEM),
        compiler_params=pltpu.CompilerParams(vmem_limit_bytes=8 * 2**20),
    )(*arrays)


def in_hbm(v):
    return pltpu.with_memory_space_constraint(v, pltpu.HBM)


def take_kernel(block, selected, inputs, out):
    row_count, width = inputs.shape
    taken = selected[...] - block[0] * row_count
    mine = (taken >= 0) & (taken < row_count)
    lower = jnp.min(jnp.where(mine, taken, row_count), axis=0, keepdims=True)
    upper = jnp.max(jnp.where(mine, taken, -1), axis=0, keepdims=True)
    upper = jnp.where(upper > lower, upper, -1)
    count = out.shape[0]
    experts = selected.shape[1]
    slot = lax.broadcasted_iota(jnp.int32, (count, experts), 0)
    expert = lax.broadcasted_iota(jnp.int32, (count, experts), 1)
    either = jnp.where(slot % 2 == 0, lower, upper)
    own = jnp.where(slot // 8 * 2 + slot % 4 // 2 == expert, either, 0)
    pick = jnp.dot(
        own.astype(jnp.float32).astype(jnp.bfloat16),
        jnp.ones((experts, row_count), jnp.bfloat16),
        preferred_element_type=jnp.float32,
    ).astype(jnp.int32)
    slot = lax.broadcasted_iota(jnp.int32, (count, row_count), 0)
    row = lax.broadcasted_iota(jnp.int32, (count, row_count), 1)
    hit = pick == row
    left = jnp.where(hit & (slot % 8 < 4), 1.0, 0.0).astype(jnp.bfloat16)
    right = jnp.where(hit & (slot % 8 >= 4), 1.0, 0.0).astype(jnp.bfloat16)
    half = width // 2
    out[...] = (
        jnp.dot(left, inputs[:, :half], preferred_element_type=jnp.float32)
        + jnp.dot(right, inputs[:, half:], preferred_element_type=jnp.float32)
    ).astype(out.dtype)


def fill_kernel(place, arrived, out):
    slots, half = place.shape[0], arrived.shape[1]
    source = lax.broadcasted_iota(jnp.int32, (slots, arrived.shape[0]), 1)
    for h in range(2):
        hit = jnp.where(source == place[...] + 4 * h, 1.0, 0.0).astype(jnp.bfloat16)
        rows = jnp.dot(hit, arrived[...], preferred_element_type=jnp.float32).astype(out.dtype)
        for c in range(out.shape[0]):
            out[c, :, h * half : (h + 1) * half] = rows


def reply_kernel(place, gate, parts, out):
    total = parts[0].astype(jnp.float32)
    for c in range(1, parts.shape[0]):
        total = total + parts[c].astype(jnp.float32)
    weighted = (total * gate[...]).astype(jnp.bfloat16)
    half = out.shape[1]
    target = lax.broadcasted_iota(jnp.int32, (out.shape[0], place.shape[1]), 0)
    left = jnp.where(target == place[...], 1.0, 0.0).astype(jnp.bfloat16)
    right = jnp.where(target == place[...] + 4, 1.0, 0.0).astype(jnp.bfloat16)
    out[...] = (
        jnp.dot(left, weighted[:, :half], preferred_element_type=jnp.float32)
        + jnp.dot(right, weighted[:, half:], preferred_element_type=jnp.float32)
    ).astype(out.dtype)


def join_kernel(pieces, out):
    width = pieces.shape[2]
    for c in range(pieces.shape[0]):
        out[:, c * width : (c + 1) * width] = pieces[c]


def expert_kernel(chosen, gate, up, down, out, down_here, sems):
    senders, _, width = chosen.shape
    experts = gate.shape[0]
    take = chosen.shape[1] // experts
    moves = [
        pltpu.make_async_copy(down.at[x], down_here.at[x], sems.at[x]) for x in range(experts)
    ]
    for move in moves:
        move.start()
    for x in range(experts):
        slots = slice(x * take, (x + 1) * take)
        rows = chosen[:, slots, :].reshape(senders * take, width)
        gate_part = jnp.dot(rows, gate[x], preferred_element_type=jnp.float32)
        up_part = jnp.dot(rows, up[x], preferred_element_type=jnp.float32)
        hidden = (gate_part / (1.0 + jnp.exp(-gate_part)) * up_part).astype(jnp.bfloat16)
        moves[x].wait()
        partial = jnp.dot(hidden, down_here[x], preferred_element_type=jnp.float32)
        out[:, slots, :] = partial.astype(jnp.bfloat16).reshape(senders, take, width)


def expert_parts(chosen, gate, up, down):
    vmem = pl.BlockSpec(memory_space=pltpu.VMEM)
    return pl.pallas_call(
        expert_kernel,
        out_shape=jax.ShapeDtypeStruct(chosen.shape, chosen.dtype),
        in_specs=[vmem, vmem, vmem, pl.BlockSpec(memory_space=pltpu.HBM)],
        out_specs=vmem,
        scratch_shapes=[
            pltpu.VMEM(down.shape, down.dtype),
            pltpu.SemaphoreType.DMA((down.shape[0],)),
        ],
        compiler_params=pltpu.CompilerParams(vmem_limit_bytes=12 * 2**20),
        name="experts",
    )(chosen, gate, up, in_hbm(down))


def attention_kernel(ids, train, near, far, out, queries, keys, values):
    rows, width = 128, 2 * HEAD_DIM
    half = near.shape[0] // rows
    chunks = 2 * half
    lane = lax.broadcasted_iota(jnp.int32, (rows, width), 1)
    first = lane < HEAD_DIM
    one_lane = jnp.where(lane == 0, 1.0, 0.0).astype(jnp.bfloat16)
    for j in range(chunks):
        source = near if j < half else far
        at = (j % half) * rows
        here = slice(j * rows, (j + 1) * rows)
        low, high = slice(2 * j * rows, (2 * j + 1) * rows), slice((2 * j + 1) * rows, (2 * j + 2) * rows)
        q = source[at : at + rows, 0:width]
        zero = jnp.zeros_like(q)
        queries[low, 0:width] = jnp.where(first, q, zero)
        queries[high, 0:width] = jnp.where(first, zero, q)
        queries[low, width:] = one_lane
        queries[high, width:] = one_lane
        position = ids[j] * rows + lax.broadcasted_iota(jnp.int32, (rows, width), 0)
        masked = (position >= train[0]) & (lane == 0)
        keys[here, 0:width] = source[at : at + rows, width : 2 * width]
        keys[here, width:] = jnp.where(masked, MASKED, 0.0).astype(jnp.bfloat16)
        values[here, 0:width] = source[at : at + rows, 2 * width : 3 * width]
        values[here, width:] = jnp.ones((rows, width), jnp.bfloat16)

    for j in range(chunks):
        q = queries[2 * j * rows : (2 * j + 2) * rows, :]
        scores = lax.dot_general(
            q, keys[...], (((1,), (1,)), ((), ())), preferred_element_type=jnp.float32
        )
        top = jnp.max(scores, axis=1, keepdims=True)
        weights = jnp.exp2((scores - top) * (LOG2_E * HEAD_DIM**-0.5)).astype(jnp.bfloat16)
        mixed = jnp.dot(weights, values[...], preferred_element_type=jnp.float32)
        blended = mixed[:, :width] / mixed[:, width:]
        out[ids[j]] = jnp.where(first, blended[:rows], blended[rows:]).astype(jnp.bfloat16)


def attention(ids, train, near, far):
    chunks = ids.shape[0]
    rows, width = 128, 2 * HEAD_DIM
    vmem = pl.BlockSpec(memory_space=pltpu.VMEM)
    smem = pl.BlockSpec(memory_space=pltpu.SMEM)
    return pl.pallas_call(
        attention_kernel,
        out_shape=jax.ShapeDtypeStruct((chunks, rows, width), jnp.bfloat16),
        in_specs=[smem, smem, vmem, vmem],
        out_specs=vmem,
        scratch_shapes=[
            pltpu.VMEM((2 * chunks * rows, 2 * width), jnp.bfloat16),
            pltpu.VMEM((chunks * rows, 2 * width), jnp.bfloat16),
            pltpu.VMEM((chunks * rows, 2 * width), jnp.bfloat16),
        ],
        compiler_params=pltpu.CompilerParams(vmem_limit_bytes=20 * 2**20),
        name="attention",
    )(ids, train, near, far)


def local(
    inputs,
    selected,
    selection_gate,
    gate_weight,
    up_weight,
    down_weight,
    norm_gain,
    query_weight,
    key_weight,
    value_weight,
    train_count,
):
    exp_count = lax.axis_size("exp")
    ctx_count = lax.axis_size("ctx")
    exp_index = lax.axis_index("exp")
    ctx_index = lax.axis_index("ctx")
    row_count, model_width = inputs.shape
    experts = gate_weight.shape[0]
    group_take = selected.shape[1]
    table_rows = row_count * ctx_count
    head_width = model_width // ctx_count

    piece = jnp.concatenate(
        [
            lax.dynamic_slice_in_dim(w, ctx_index * head_width, head_width, 1)
            for w in (query_weight, key_weight, value_weight)
        ],
        axis=1,
    )
    own_block = exp_index * ctx_count + ctx_index
    half = model_width // 2
    sent = (exp_count, 2 * experts * MOST, half)
    flat = jax.ShapeDtypeStruct((sent[0] * sent[1], half), inputs.dtype)
    outgoing = small_kernel(
        take_kernel, flat, own_block.reshape(1), in_hbm(selected.T), in_hbm(inputs), scalars=1
    )
    arrived = exchange(outgoing.reshape(sent), "exp").reshape(flat.shape)
    taken = selected.reshape(exp_count, experts, group_take) - own_block * row_count
    mine = (taken >= 0) & (taken < row_count)
    lower = jnp.min(jnp.where(mine, taken, row_count), axis=2)
    upper = jnp.max(jnp.where(mine, taken, -1), axis=2)
    upper = jnp.where(upper > lower, upper, -1)
    lower = jnp.where(lower < row_count, lower, -1)
    picks = jnp.stack([lower, upper], axis=2).reshape(exp_count, 1, experts * MOST)
    halves = jnp.arange(2, dtype=jnp.int32)[None, :, None] * row_count
    picks = jnp.where(picks < 0, -1, picks + halves).reshape(-1, 1)
    row_ids = jnp.arange(2 * row_count, dtype=jnp.int32)
    owner_hit = (picks == row_ids).astype(jnp.bfloat16)

    my_rows = lax.dynamic_slice_in_dim(selected, exp_index * experts, experts, 0)
    my_table = my_rows // table_rows
    lower_rows = (my_table[:, :, None] == my_table[:, None, :]) & (
        my_rows[:, None, :] < my_rows[:, :, None]
    )
    my_rank = jnp.sum(lower_rows.astype(jnp.int32), axis=2)
    expert_ids = jnp.arange(experts, dtype=jnp.int32)[:, None]
    my_place = (my_table * sent[1] + expert_ids * MOST + my_rank).reshape(-1)
    gates = selection_gate.reshape(-1, 1)

    chosen_shape = jax.ShapeDtypeStruct(
        (ctx_count, experts * group_take, model_width), inputs.dtype
    )
    compact = small_kernel(fill_kernel, chosen_shape, my_place.reshape(-1, 1), arrived)
    chosen = exchange(compact, "ctx")
    quarter = gather_four(piece, exp_index // 4 % 4, 4, compact)
    layer = jnp.moveaxis(gather_four(quarter, exp_index % 4, 1), 0, 1)
    partials = expert_parts(chosen, gate_weight, up_weight, down_weight)
    parts = exchange(partials, "ctx")
    reply = small_kernel(reply_kernel, flat, my_place.reshape(1, -1), gates, parts)
    reply, layer = lax.optimization_barrier((reply, layer))
    returned = exchange(reply.reshape(sent), "exp").reshape(flat.shape)
    weight_rows = gather_four(layer, exp_index // N_Z, N_Z).reshape(model_width, -1)
    sums = lax.dot_general(
        owner_hit, returned, (((0,), (0,)), ((), ())), preferred_element_type=jnp.float32
    )
    moe_sum = jnp.concatenate([sums[:row_count], sums[row_count:]], axis=1)

    layer_out = (inputs.astype(jnp.float32) + moe_sum).astype(jnp.bfloat16)
    widened = layer_out.astype(jnp.float32)
    scale_row = lax.rsqrt(jnp.mean(widened * widened, axis=1, keepdims=True) + EPSILON)
    normed = (widened * scale_row * norm_gain).astype(jnp.bfloat16)

    near = jnp.concatenate(
        [normed, shift_chip(normed, 2), shift_chip(normed, 1), shift_chip(normed, -1)], axis=0
    )
    far = swap_core(near)
    chip, core = ctx_index // N_CORE, ctx_index % N_CORE
    steps = jnp.array([0, 2, N_X - 1, 1], jnp.int32)
    chips = (chip + steps) % N_X
    ids = jnp.concatenate([chips * N_CORE + core, chips * N_CORE + 1 - core])
    near_rows = jnp.dot(near, weight_rows, preferred_element_type=jnp.float32)
    far_rows = jnp.dot(far, weight_rows, preferred_element_type=jnp.float32)
    mixed = attention(
        ids, train_count, near_rows.astype(jnp.bfloat16), far_rows.astype(jnp.bfloat16)
    )
    by_heads = exchange(mixed, "ctx")
    context = small_kernel(join_kernel, jax.ShapeDtypeStruct(inputs.shape, inputs.dtype), by_heads)
    return (layer_out, context)


def solution(mesh):
    placed = (
        P(("exp", "ctx"), None),
        P(None, "ctx"),
        P("exp", "ctx"),
        P("exp", None, "ctx"),
        P("exp", None, "ctx"),
        P("exp", "ctx", None),
        P(),
        P("exp", None),
        P("exp", None),
        P("exp", None),
        P("exp"),
    )
    return jax.shard_map(
        local,
        mesh=mesh,
        in_specs=placed,
        out_specs=(P(("exp", "ctx"), None), P(("exp", "ctx"), None)),
        check_vma=False,
    )
```
